32 devices in a mesh: tm: 8 (over z, y), space: 4 (over x, core).
Axes of the slice: x: 2, y: 2, z: 4, core: 2. Of those that a mesh axis runs over, the one named last changes fastest.
Arguments:
- initial: float32 [8, 128, 128], P('space'), may hold values from -6 to 6
- start_guess: float32 [8, 8, 128, 128], P('tm', 'space'), may hold values from -6 to 6
- forcing: float32 [8, 5, 8, 128, 128], P('tm', None, 'space'), may hold values from -6 to 6
- step_size: float32 [8], P('tm'), may hold values from 0.06 to 0.16
Outputs:
- fine_values: float32 [8, 5, 8, 128, 128], P('tm', None, 'space')
The draws below stay inside these ranges and needn't reach their ends.
All inputs are finite; a program needn't handle non-finite values.
Results may differ from the reference program's by a relative error of at most 0.0001.
Values sent between devices are 32-bit elements; how exact they have to be, the bound alone decides.
A program may use at most 64 MiB of HBM per device.

```python
import math
import jax
import jax.numpy as jnp
import numpy as np
from jax import lax

NX = 128
NY = 128
NODES = 5
ITERS = 2
NTIME = 8
NZ = 8


def level_of(rng, shape, cuts, low, top_value):
    gain, own = 1.0, jax.random.fold_in(rng, 6)
    for axis_at, blocks in cuts:
        steps = jnp.exp(jax.random.uniform(jax.random.fold_in(own, axis_at), (blocks,), jnp.float32, low / len(cuts), top_value / len(cuts)))
        gain = gain * jnp.repeat(steps, shape[axis_at] // blocks).reshape([-1 if axis == axis_at else 1 for axis in range(len(shape))])
    return gain


def centred(stream_key, shape, scale, bound, shards=(), kind=jnp.bfloat16):
    result = scale * jax.random.normal(stream_key, shape, jnp.float32)
    if shards:
        result = result * level_of(stream_key, shape, shards, -0.22, 0.18)
    return jnp.clip(result, -bound, bound).astype(kind)


def setup_inputs(seed: int = 0) -> dict:
    arg_keys = jax.random.split(jax.random.key(seed), 5)
    return {
        "initial": centred(arg_keys[0], (NZ, NX, NY), 1.0, 6.0, ((0, 4),), jnp.float32),
        "start_guess": centred(arg_keys[1], (NTIME, NZ, NX, NY), 1.0, 6.0, ((0, 8), (1, 4)), jnp.float32),
        "forcing": centred(arg_keys[2], (NTIME, NODES, NZ, NX, NY), 1.0, 6.0, ((0, 8), (2, 4)), jnp.float32),
        "step_size": jnp.clip(jnp.exp(math.log(0.16) - 0.98082925 * jax.random.uniform(arg_keys[3], (NTIME,), jnp.float32) ** level_of(arg_keys[3], (NTIME,), ((0, 8),), -0.2, 0.2)), 0.06, 0.16),
    }


def node_tables():
    radical = math.sqrt(3.0 / 7.0)
    node_times = [0.0, (1.0 - radical) / 2.0, 0.5, (1.0 + radical) / 2.0, 1.0]
    integrals = np.zeros((4, 5))
    for column in range(5):
        coeffs = [1.0]
        for other_index in range(5):
            if other_index == column:
                continue
            other_time = node_times[other_index]
            scaling = node_times[column] - other_time
            grown = [0.0] * (len(coeffs) + 1)
            for exponent in range(len(coeffs)):
                grown[exponent + 1] += coeffs[exponent] / scaling
                grown[exponent] -= coeffs[exponent] * other_time / scaling
            coeffs = grown
        for section in range(4):
            integrals[section, column] = sum((coeffs[exponent] * (node_times[section + 1] ** (exponent + 1) - node_times[section] ** (exponent + 1)) / (exponent + 1) for exponent in range(len(coeffs))))
    coarse = [0.0, 0.5, 1.0]
    interp = np.zeros((5, 3))
    for column in range(3):
        for section in range(5):
            weight = 1.0
            for other_index in range(3):
                if other_index != column:
                    weight = weight * (node_times[section] - coarse[other_index]) / (coarse[column] - coarse[other_index])
            interp[section, column] = weight
    return (np.array(node_times), integrals, interp)

def laplace(field):
    widths = [(0, 0)] * (field.ndim - 3) + [(1, 1)] * 3
    padded = jnp.pad(field, widths)
    center = padded[..., 1:-1, 1:-1, 1:-1]
    return padded[..., 2:, 1:-1, 1:-1] + padded[..., :-2, 1:-1, 1:-1] + padded[..., 1:-1, 2:, 1:-1] + padded[..., 1:-1, :-2, 1:-1] + padded[..., 1:-1, 1:-1, 2:] + padded[..., 1:-1, 1:-1, :-2] - 6.0 * center

def fine_sweep(values, forcing, full_step, node_times, integrals):
    half_step = 0.5 * full_step
    lap_old = laplace(values)
    rates = lap_old + forcing
    swept = [values[0]]
    lap_new = [lap_old[0]]
    for section in range(4):
        quadrature = sum((float(integrals[section, column]) * rates[column] for column in range(5)))
        spacing = float(node_times[section + 1] - node_times[section])
        advanced = swept[section] + full_step * spacing * (lap_new[section] - lap_old[section]) + full_step * quadrature
        swept.append(advanced)
        lap_new.append(laplace(advanced))
    new_rates = [lap_new[column] + forcing[column] for column in range(5)]
    first_half = full_step * sum((float(integrals[0, column] + integrals[1, column]) * new_rates[column] for column in range(5)))
    second_half = full_step * sum((float(integrals[2, column] + integrals[3, column]) * new_rates[column] for column in range(5)))
    left = first_half - half_step * lap_new[0]
    right = second_half - half_step * lap_new[2]
    return (jnp.stack(swept), left, right)

def reference(initial, start_guess, forcing, step_size):
    node_times, integrals, interp = node_tables()
    values = jnp.broadcast_to(start_guess[:, None], (NTIME, NODES, NZ, NX, NY))

    def link(start_value, packed):
        left_term, right_term, half_step = packed
        middle = start_value + half_step * laplace(start_value) + left_term
        ending = middle + half_step * laplace(middle) + right_term
        return (ending, (start_value, middle, ending))
    for sweep_round in range(ITERS):
        starts = jnp.concatenate([initial[None], values[:-1, NODES - 1]], axis=0)
        values = values.at[:, 0].set(starts)
        swept, left, right = lax.map(lambda packed: fine_sweep(packed[0], packed[1], packed[2], node_times, integrals), (values, forcing, step_size))
        last_value, coarse = lax.scan(link, initial, (left, right, 0.5 * step_size))
        deltas = [coarse[0] - swept[:, 0], coarse[1] - swept[:, 2], coarse[2] - swept[:, 4]]
        values = jnp.stack([swept[:, section] + sum((float(interp[section, column]) * deltas[column] for column in range(3))) for section in range(5)], axis=1)
    return values
```

```python
import functools
import math

import jax
import jax.numpy as jnp
import numpy as np
from jax import lax
from jax.experimental import pallas as pl
from jax.experimental.pallas import tpu as pltpu
from jax.sharding import PartitionSpec as P

MESH = pl.DeviceIdType.MESH
CHUNKS = 4
UNROLL = 8

def node_tables():
    radical = math.sqrt(3.0 / 7.0)
    node_times = [0.0, (1.0 - radical) / 2.0, 0.5, (1.0 + radical) / 2.0, 1.0]
    integrals = np.zeros((4, 5))
    for column in range(5):
        coeffs = [1.0]
        for other_index in range(5):
            if other_index == column:
                continue
            other_time = node_times[other_index]
            scaling = node_times[column] - other_time
            grown = [0.0] * (len(coeffs) + 1)
            for exponent in range(len(coeffs)):
                grown[exponent + 1] += coeffs[exponent] / scaling
                grown[exponent] -= coeffs[exponent] * other_time / scaling
            coeffs = grown
        for section in range(4):
            integrals[section, column] = sum(
                (
                    coeffs[exponent]
                    * (
                        node_times[section + 1] ** (exponent + 1)
                        - node_times[section] ** (exponent + 1)
                    )
                    / (exponent + 1)
                    for exponent in range(len(coeffs))
                )
            )
    coarse = [0.0, 0.5, 1.0]
    interp = np.zeros((5, 3))
    for column in range(3):
        for section in range(5):
            weight = 1.0
            for other_index in range(3):
                if other_index != column:
                    weight = (
                        weight
                        * (node_times[section] - coarse[other_index])
                        / (coarse[column] - coarse[other_index])
                    )
            interp[section, column] = weight
    return (np.array(node_times), integrals, interp)


def sine(length):
    k = np.arange(1, length + 1)
    phase = np.outer(k, k) % (2 * (length + 1))
    return math.sqrt(2.0 / (length + 1)) * np.sin(math.pi / (length + 1) * phase)


def eigen(length):
    return 2.0 - 2.0 * np.cos(math.pi / (length + 1) * np.arange(1, length + 1))


def split_pair(value):
    high = value.astype(jnp.bfloat16)
    return high, (value - high.astype(jnp.float32)).astype(jnp.bfloat16)


def dot(a, b):
    return jnp.dot(a, b, preferred_element_type=jnp.float32)


def along_y(field, w_ref):
    width = field.shape[1]
    both = dot(jnp.concatenate(split_pair(field), axis=1), w_ref[...])
    return both[:, :width] + both[:, width:]


def along_x(pair, high, x_ref, low_ref):
    return dot(x_ref[...], pair) + dot(low_ref[...], high)


def lateral(field, x_ref, low_ref, w_ref):
    depth, width_x, width_y = field.shape
    mixed = along_y(field.reshape(depth * width_x, width_y), w_ref)
    mixed = jnp.concatenate([mixed[z * width_x : (z + 1) * width_x] for z in range(depth)], axis=1)
    high, low = split_pair(mixed)
    out = along_x(jnp.concatenate([high, low], axis=0), high, x_ref, low_ref)
    return [out[:, z * width_y : (z + 1) * width_y] for z in range(depth)]


def z_sine(planes):
    count = len(planes)
    table = sine(count)
    half = (count + 1) // 2
    pairs = [
        (planes[z] + planes[count - 1 - z], planes[z] - planes[count - 1 - z])
        if z != count - 1 - z
        else (planes[z], None)
        for z in range(half)
    ]
    out = []
    for k in range(count):
        terms = [
            float(table[k, z]) * pairs[z][k % 2] for z in range(half) if pairs[z][k % 2] is not None
        ]
        total = terms[0]
        for term in terms[1:]:
            total = total + term
        out.append(total)
    return out


def weighted(weights, items):
    total = None
    for weight, item in zip(weights, items):
        weight = float(weight)
        if weight == 0.0 or item is None:
            continue
        term = item if weight == 1.0 else weight * item
        total = term if total is None else total + term
    return total


def sweep(rate, nodes, sources):
    times, integrals, _ = TABLES
    swept = [nodes[0]]
    for m in range(4):
        spacing = float(times[m + 1] - times[m])
        inner = weighted(integrals[m], nodes)
        if m > 0:
            inner = inner + spacing * (swept[m] - nodes[m])
        step = rate * inner
        if swept[m] is not None:
            step = step + swept[m]
        if sources is not None:
            step = step + sources[m]
        swept.append(step)
    first = list(integrals[0] + integrals[1])
    second = list(integrals[2] + integrals[3])
    first[0] -= 0.5
    second[2] -= 0.5
    left = rate * weighted(first, swept)
    right = rate * weighted(second, swept)
    if sources is not None:
        left = left + (sources[0] + sources[1])
        right = right + (sources[2] + sources[3])
    return swept, left, right


def corrected(swept, left, right, middle):
    interp = TABLES[2]
    ending = middle * left + right
    deltas = [None if swept[0] is None else -swept[0], left - swept[2], ending - swept[4]]
    return [
        None,
        swept[1] + weighted(interp[1], deltas),
        left,
        swept[3] + weighted(interp[3], deltas),
        ending,
    ]


def start_gains(middle):
    interp = TABLES[2]
    square = middle * middle
    return [
        None,
        float(interp[1, 0]) + float(interp[1, 1]) * middle + float(interp[1, 2]) * square,
        middle,
        float(interp[3, 0]) + float(interp[3, 1]) * middle + float(interp[3, 2]) * square,
        square,
    ]


def gains_of(rate):
    middle = 1.0 + 0.5 * rate
    gains = start_gains(middle)
    nodes = [jnp.ones_like(middle)] + gains[1:]
    swept, left, right = sweep(rate, nodes, None)
    return gains, corrected(swept, left, right, middle)


TABLES = node_tables()


def kernel(
    dims,
    step_ref, initial_hbm, guess_hbm, forcing_hbm, x_hbm, low_hbm, w_hbm, lateral_hbm,
    result_ref,
    initial, guess, forcing, x_ref, low_ref, w_ref, lateral_ref,
    in_send, in_recv, ghat, hhat, ell, own_step, steps,
    gain_c, gain_d, part_b, z_send, z_recv, own_gain, own_cross, r_send, r_recv,
    o_send, o_recv, mix,
    load_sem, in_ss, in_rs, h_ss, h_rs, s_ss, s_rs, z_ss, z_rs, r_ss, r_rs, o_ss, o_rs,
    near_sem, next_sem, open_sem,
):
    spaces, slices, chunks, depth, length_z, rows, width_y, owners, block = dims
    me = lax.axis_index("space")
    place = lax.axis_index("tm")
    _, integrals, _ = TABLES
    width_x = spaces * chunks * rows
    everyone = spaces - 2

    barrier = pltpu.get_barrier_semaphore()
    odd = lax.rem(me, 2) == 1
    for i in range(1, spaces):
        peer = lax.rem(me + i, spaces)

        @pl.when(lax.rem(peer, 2) == 1)
        def _():
            pl.semaphore_signal(barrier, inc=1, device_id={"space": peer}, device_id_type=MESH)

    sources = (
        guess_hbm.at[0], w_hbm, x_hbm, low_hbm, forcing_hbm.at[0], initial_hbm, lateral_hbm
    )
    loads = [
        pltpu.make_async_copy(source, target, load_sem.at[i])
        for i, (source, target) in enumerate(
            zip(sources, (guess, w_ref, x_ref, low_ref, forcing, initial, lateral_ref))
        )
    ]
    for load in loads:
        load.start()
    load_guess, load_w, load_x, load_low, load_forcing, load_initial, load_lateral = loads

    step = step_ref[0]
    own_step[...] = jnp.full(own_step.shape, step, jnp.float32)
    steps[place] = jnp.full(own_step.shape, step, jnp.float32)

    def low_of(c, s):
        return (c * spaces + s) * rows

    def put(field, slot):
        planes = lateral(field, x_ref, low_ref, w_ref)
        for target in range(spaces):
            for c in range(chunks):
                low = low_of(c, target)
                for z in range(depth):
                    in_send[c, target, slot, z] = planes[z][low : low + rows]

    def keep(c, low, high):
        in_recv[c, me, low:high] = in_send[c, me, low:high]

    groups = ((0, 1), (1, 5), (5, 6))

    def in_copy(c, group, peer, source):
        low, high = groups[group]
        return pltpu.make_async_remote_copy(
            src_ref=in_send.at[c, peer, low:high],
            dst_ref=in_recv.at[c, source, low:high],
            send_sem=in_ss.at[c, group, peer],
            recv_sem=in_rs.at[c, group, source],
            device_id={"space": peer},
            device_id_type=MESH,
        )

    def in_start(c, group):
        for i in range(1, spaces):
            in_copy(c, group, lax.rem(me + i, spaces), me).start()

    def in_wait(c, group):
        for i in range(1, spaces):
            peer = lax.rem(me + i, spaces)
            in_copy(c, group, peer, peer).wait_recv()

    load_guess.wait()
    load_w.wait()
    load_x.wait()
    load_low.wait()
    put(guess[...], 0)

    @pl.when(odd)
    def _():
        pl.semaphore_wait(barrier, spaces - 1)
        pl.semaphore_signal(near_sem, inc=1, device_id={"space": me - 1}, device_id_type=MESH)

    @pl.when(jnp.logical_not(odd))
    def _():
        pl.semaphore_wait(near_sem, 1)

    for c in range(min(2, chunks)):
        in_start(c, 0)

    @pl.when(jnp.logical_and(me == 0, place > 0))
    def _():
        pl.semaphore_signal(barrier, inc=1, device_id={"tm": place - 1}, device_id_type=MESH)

    def peers(action):
        def one(i, carry):
            action(lax.rem(place + i, slices))
            return carry

        if slices > UNROLL:
            lax.fori_loop(1, slices, one, 0)
        else:
            for i in range(1, slices):
                one(i, 0)

    @pl.when(me == everyone)
    def _():
        peers(
            lambda peer: pl.semaphore_signal(
                barrier, inc=1, device_id={"tm": peer}, device_id_type=MESH
            )
        )

    def tell(sem):
        for i in range(1, spaces):
            pl.semaphore_signal(
                sem, inc=1, device_id={"space": lax.rem(me + i, spaces)}, device_id_type=MESH
            )

    for c in range(chunks):
        keep(c, 0, 1)
    load_forcing.wait()
    for m in range(4):
        put(step * weighted(integrals[m], [forcing[j] for j in range(5)]), m + 1)

    load_initial.wait()

    @pl.when(place == 0)
    def _():
        put(initial[...], 5)

    for c in range(chunks):
        in_start(c, 1)

        @pl.when(place == 0)
        def _():
            in_start(c, 2)

        if c + 2 < chunks:
            in_start(c + 2, 0)
    for c in range(chunks):
        keep(c, 1, 5)

        @pl.when(place == 0)
        def _():
            keep(c, 5, 6)

    @pl.when(place < slices - 1)
    def _():
        @pl.when(me == 0)
        def _():
            pl.semaphore_wait(barrier, 1)
            tell(next_sem)

    z_eigen = eigen(length_z)
    load_lateral.wait()
    for c in range(chunks):
        low = pl.multiple_of(low_of(c, me), 8)
        base = lateral_ref[pl.ds(low, rows), :]
        for k in range(length_z):
            ell[c, k * rows : (k + 1) * rows] = -(base + float(z_eigen[k]))

    def table(i, carry):
        for c in range(chunks):
            at = pl.ds(pl.multiple_of(i * rows, 8), rows)
            gains, crossed = gains_of(step * ell[c, at])
            for m in range(1, 5):
                gain_c[c, m - 1, at] = gains[m]
                gain_d[c, m - 1, at] = crossed[m]
        return carry

    lax.fori_loop(0, length_z, table, 0)

    def planes_of(c, slot):
        return [in_recv[c, z // depth, slot, z % depth] for z in range(length_z)]

    def h_copy(c, peer):
        return pltpu.make_async_remote_copy(
            src_ref=ghat.at[c],
            dst_ref=hhat.at[c],
            send_sem=h_ss.at[c],
            recv_sem=h_rs.at[c],
            device_id={"tm": peer},
            device_id_type=MESH,
        )

    after = lax.rem(place + 1, slices)

    def hand(c):
        in_wait(c, 0)
        for k, plane in enumerate(z_sine(planes_of(c, 0))):
            ghat[c, k * rows : (k + 1) * rows] = plane

        @pl.when(place < slices - 1)
        def _():
            h_copy(c, after).start()

    @pl.when(jnp.logical_and(place < slices - 1, me != 0))
    def _():
        pl.semaphore_wait(next_sem, 1)

    def step_copy(peer, source):
        return pltpu.make_async_remote_copy(
            src_ref=own_step,
            dst_ref=steps.at[source],
            send_sem=s_ss.at[peer],
            recv_sem=s_rs.at[source],
            device_id={"tm": peer},
            device_id_type=MESH,
        )

    def z_copy(c, owner, source):
        return pltpu.make_async_remote_copy(
            src_ref=z_send.at[c, owner],
            dst_ref=z_recv.at[c, source],
            send_sem=z_ss.at[c],
            recv_sem=z_rs.at[c, source],
            device_id={"tm": owner},
            device_id_type=MESH,
        )

    def to_owner(owner, action):
        if owners == slices:
            action()
        else:
            pl.when(owner < owners)(action)

    def bulk_wait(ref, sem, count):
        if count > 0:
            pltpu.make_async_copy(ref.at[0:count], ref.at[0:count], sem).wait()

    def owner_wait(ref, sem):
        if owners == slices:
            bulk_wait(ref, sem, owners - 1)
        else:
            pl.when(place < owners)(lambda: bulk_wait(ref, sem, owners - 1))
            pl.when(place >= owners)(lambda: bulk_wait(ref, sem, owners))

    def opened():
        @pl.when(me == everyone)
        def _():
            pl.semaphore_wait(barrier, slices - 1)
            tell(open_sem)

        @pl.when(me != everyone)
        def _():
            pl.semaphore_wait(open_sem, 1)

        peers(lambda peer: step_copy(peer, place).start())

    first = jnp.where(place == 0, 1.0, 0.0).astype(jnp.float32)
    hand(0)
    for c in range(chunks):
        if c + 1 < chunks:
            hand(c + 1)
        in_wait(c, 1)
        fhat = [z_sine(planes_of(c, m + 1)) for m in range(4)]
        for m in range(4):
            for k in range(length_z):
                part_b[c, m, k * rows : (k + 1) * rows] = fhat[m][k]

        @pl.when(place == 0)
        def _():
            in_wait(c, 2)
            for k, plane in enumerate(z_sine(planes_of(c, 5))):
                hhat[c, k * rows : (k + 1) * rows] = plane

        @pl.when(place > 0)
        def _():
            h_copy(c, after).wait_recv()

        def solve(i, carry):
            at = pl.ds(pl.multiple_of(i * block, 8), block)
            rate = step * ell[c, at]
            middle = 1.0 + 0.5 * rate
            guess_hat, start = ghat[c, at], hhat[c, at]
            sources = [part_b[c, m, at] for m in range(4)]
            one = sweep(rate, [start] + [guess_hat] * 4, sources)
            nodes = corrected(*one, middle)
            rest = corrected(*sweep(rate, nodes, sources), middle)
            for m in range(1, 5):
                part_b[c, m - 1, at] = rest[m]
            seen = first * start
            gain, cross = gain_c[c, 3, at], gain_d[c, 3, at]
            z_send[c, i, 0] = nodes[4] + gain * seen
            z_send[c, i, 1] = rest[4] + (gain + cross) * seen
            return carry

        lax.fori_loop(0, owners, solve, 0, unroll=4)
        if c == 0:
            opened()

        @pl.when(place < slices - 1)
        def _():
            peers(lambda peer: to_owner(peer, lambda: z_copy(c, peer, place).start()))

        @pl.when(place < owners)
        def _():
            z_recv[c, place] = z_send[c, place]

    peers(lambda peer: step_copy(peer, peer).wait_recv())

    @pl.when(place < owners)
    def _():
        def one(p, carry):
            for c in range(chunks):
                at = pl.ds(pl.multiple_of(place * block, 8), block)
                gains, crossed = gains_of(steps[p][0:1] * ell[c, at])
                own_gain[c, p] = gains[4]
                own_cross[c, p] = crossed[4]
            return carry

        lax.fori_loop(0, slices - 1, one, 0)

    def r_copy(c, target, owner):
        return pltpu.make_async_remote_copy(
            src_ref=r_send.at[c, target],
            dst_ref=r_recv.at[c, owner],
            send_sem=r_ss.at[c],
            recv_sem=r_rs.at[c],
            device_id={"tm": target},
            device_id_type=MESH,
        )

    for c in range(chunks):
        @pl.when(place < owners)
        def _():
            def scan(p, state):
                @pl.when(p != place)
                def _():
                    z_copy(c, p, p).wait_recv()

                lower, upper = state
                gain = own_gain[c, p]
                lower, upper = (
                    gain * lower + z_recv[c, p, 0],
                    gain * upper + own_cross[c, p] * lower + z_recv[c, p, 1],
                )
                target = p + 1
                r_send[c, target, 0] = lower
                r_send[c, target, 1] = upper

                @pl.when(target != place)
                def _():
                    r_copy(c, target, place).start()

                @pl.when(target == place)
                def _():
                    r_recv[c, place, 0] = lower
                    r_recv[c, place, 1] = upper

                return lower, upper

            zero = jnp.zeros((block, width_y), jnp.float32)
            state = (zero, zero)
            if slices > UNROLL:
                lax.fori_loop(0, slices - 1, scan, state)
            else:
                for p in range(slices - 1):
                    state = scan(p, state)

    def o_groups(c):
        return tuple((m, m + 1) for m in range(5)) if c == chunks - 1 else ((0, 5),)

    def o_copy(c, group, peer, source):
        low, high = o_groups(c)[group]
        return pltpu.make_async_remote_copy(
            src_ref=o_send.at[c, peer, low:high],
            dst_ref=o_recv.at[c, source, low:high],
            send_sem=o_ss.at[c, group, peer],
            recv_sem=o_rs.at[c, group, source],
            device_id={"space": peer},
            device_id_type=MESH,
        )

    def o_wait(c, group):
        for i in range(1, spaces):
            peer = lax.rem(me + i, spaces)
            o_copy(c, group, peer, peer).wait_recv()

    for c in range(chunks):
        @pl.when(place > 0)
        def _():
            owner_wait(r_recv.at[c], r_rs.at[c])

        own = hhat[c].reshape(owners, block, width_y)
        lower = jnp.where(place == 0, own, r_recv[c, :, 0]).reshape(length_z * rows, width_y)
        upper = jnp.where(place == 0, own, r_recv[c, :, 1]).reshape(length_z * rows, width_y)
        for m in range(5):
            if m == 0:
                value = upper
            else:
                value = (
                    gain_c[c, m - 1] * upper + gain_d[c, m - 1] * lower + part_b[c, m - 1]
                )
            planes = z_sine([value[k * rows : (k + 1) * rows] for k in range(length_z)])
            for z in range(length_z):
                o_send[c, z // depth, m, z % depth] = planes[z]
            for group, (_, high) in enumerate(o_groups(c)):
                if high == m + 1:
                    for i in range(1, spaces):
                        o_copy(c, group, lax.rem(me + i, spaces), me).start()
            o_recv[c, me, m] = o_send[c, me, m]

    def unmix(c, low, high):
        stacked = jnp.concatenate(
            [
                o_recv[c, s, m, z]
                for m in range(low, high)
                for z in range(depth)
                for s in range(spaces)
            ],
            axis=0,
        )
        tall = spaces * rows
        mixed_high, mixed_low = split_pair(along_y(stacked, w_ref))
        for m in range(low, high):
            for z in range(depth):
                at = ((m - low) * depth + z) * tall
                lanes = slice(z * width_y, (z + 1) * width_y)
                mix[m, c * tall : (c + 1) * tall, lanes] = mixed_high[at : at + tall]
                mix[m, width_x + c * tall : width_x + (c + 1) * tall, lanes] = mixed_low[
                    at : at + tall
                ]

    for c in range(chunks - 1):
        o_wait(c, 0)
        unmix(c, 0, 5)
    for m in range(5):
        o_wait(chunks - 1, m)
        unmix(chunks - 1, m, m + 1)
        out = along_x(mix[m], mix[m, :width_x], x_ref, low_ref)
        for z in range(depth):
            result_ref[0, m, z] = out[:, z * width_y : (z + 1) * width_y]

    for c in range(chunks):
        for i in range(1, spaces):
            peer = lax.rem(me + i, spaces)
            in_copy(c, 0, peer, me).wait_send()
            in_copy(c, 1, peer, me).wait_send()

        @pl.when(place == 0)
        def _():
            for i in range(1, spaces):
                in_copy(c, 2, lax.rem(me + i, spaces), me).wait_send()

        @pl.when(place < slices - 1)
        def _():
            h_copy(c, after).wait_send()
            owner_wait(z_send.at[c], z_ss.at[c])

        @pl.when(place < owners)
        def _():
            pl.when(place == 0)(lambda: bulk_wait(r_send.at[c], r_ss.at[c], slices - 1))
            pl.when(place > 0)(lambda: bulk_wait(r_send.at[c], r_ss.at[c], slices - 2))

        for i in range(1, spaces):
            for group in range(len(o_groups(c))):
                o_copy(c, group, lax.rem(me + i, spaces), me).wait_send()

    peers(lambda peer: step_copy(peer, place).wait_send())


def body(initial, start_guess, forcing, step_size):
    depth, width_x, width_y = initial.shape
    spaces, slices = lax.axis_size("space"), lax.axis_size("tm")
    length_z = depth * spaces
    chunks = CHUNKS
    rows = width_x // spaces // chunks
    owners = min(slices, length_z * rows // 8)
    block = length_z * rows // owners
    dims = (spaces, slices, chunks, depth, length_z, rows, width_y, owners, block)

    def pair(length):
        return split_pair(jnp.asarray(sine(length), jnp.float32))

    x_high, x_low = pair(width_x)
    y_high, y_low = pair(width_y)
    x_twice = jnp.concatenate([x_high, x_high], axis=1)
    w = jnp.concatenate(
        [
            jnp.concatenate([y_high, y_low], axis=1),
            jnp.concatenate([y_high, jnp.zeros_like(y_low)], axis=1),
        ],
        axis=0,
    )
    sides = jnp.asarray(eigen(width_x)[:, None] + eigen(width_y)[None, :], jnp.float32)
    f32, b16 = jnp.float32, jnp.bfloat16
    flat = length_z * rows
    dma = pltpu.SemaphoreType.DMA
    regular = pltpu.SemaphoreType.REGULAR
    vmem = pl.BlockSpec(memory_space=pltpu.VMEM)
    hbm = pl.BlockSpec(memory_space=pl.ANY)
    return pl.pallas_call(
        functools.partial(kernel, dims),
        out_shape=pltpu.VMEM((1, 5, depth, width_x, width_y), f32),
        in_specs=[pl.BlockSpec(memory_space=pltpu.SMEM)] + [hbm] * 7,
        out_specs=vmem,
        scratch_shapes=[
            pltpu.VMEM((depth, width_x, width_y), f32),
            pltpu.VMEM((depth, width_x, width_y), f32),
            pltpu.VMEM((5, depth, width_x, width_y), f32),
            pltpu.VMEM((width_x, 2 * width_x), b16),
            pltpu.VMEM((width_x, width_x), b16),
            pltpu.VMEM((2 * width_y, 2 * width_y), b16),
            pltpu.VMEM((width_x, width_y), f32),
            pltpu.VMEM((chunks, spaces, 6, depth, rows, width_y), f32),
            pltpu.VMEM((chunks, spaces, 6, depth, rows, width_y), f32),
            pltpu.VMEM((chunks, flat, width_y), f32),
            pltpu.VMEM((chunks, flat, width_y), f32),
            pltpu.VMEM((chunks, flat, width_y), f32),
            pltpu.VMEM((8, width_y), f32),
            pltpu.VMEM((slices, 8, width_y), f32),
            pltpu.VMEM((chunks, 4, flat, width_y), f32),
            pltpu.VMEM((chunks, 4, flat, width_y), f32),
            pltpu.VMEM((chunks, 4, flat, width_y), f32),
            pltpu.VMEM((chunks, owners, 2, block, width_y), f32),
            pltpu.VMEM((chunks, slices, 2, block, width_y), f32),
            pltpu.VMEM((chunks, slices, block, width_y), f32),
            pltpu.VMEM((chunks, slices, block, width_y), f32),
            pltpu.VMEM((chunks, slices, 2, block, width_y), f32),
            pltpu.VMEM((chunks, owners, 2, block, width_y), f32),
            pltpu.VMEM((chunks, spaces, 5, depth, rows, width_y), f32),
            pltpu.VMEM((chunks, spaces, 5, depth, rows, width_y), f32),
            pltpu.VMEM((5, 2 * width_x, depth * width_y), b16),
            dma((7,)),
            dma((chunks, 3, spaces)),
            dma((chunks, 3, spaces)),
            dma((chunks,)),
            dma((chunks,)),
            dma((slices,)),
            dma((slices,)),
            dma((chunks,)),
            dma((chunks, slices)),
            dma((chunks,)),
            dma((chunks,)),
            dma((chunks, 5, spaces)),
            dma((chunks, 5, spaces)),
            regular,
            regular,
            regular,
        ],
        compiler_params=pltpu.CompilerParams(collective_id=0, has_side_effects=True),
    )(step_size, initial, start_guess, forcing, x_twice, x_low, w, sides)


def solution(mesh):
    in_specs = (
        P("space", None, None),
        P("tm", "space", None, None),
        P("tm", None, "space", None, None),
        P("tm"),
    )
    out_specs = P("tm", None, "space", None, None)
    return jax.shard_map(body, mesh=mesh, in_specs=in_specs, out_specs=out_specs, check_vma=False)
```

```python
import functools
import math

import jax
import jax.numpy as jnp
import numpy as np
from jax import lax
from jax.experimental import pallas as pl
from jax.experimental.pallas import tpu as pltpu
from jax.sharding import PartitionSpec as P

MESH = pl.DeviceIdType.MESH
CHUNKS = 4
GROUP = 8

def node_tables():
    radical = math.sqrt(3.0 / 7.0)
    node_times = [0.0, (1.0 - radical) / 2.0, 0.5, (1.0 + radical) / 2.0, 1.0]
    integrals = np.zeros((4, 5))
    for column in range(5):
        coeffs = [1.0]
        for other_index in range(5):
            if other_index == column:
                continue
            other_time = node_times[other_index]
            scaling = node_times[column] - other_time
            grown = [0.0] * (len(coeffs) + 1)
            for exponent in range(len(coeffs)):
                grown[exponent + 1] += coeffs[exponent] / scaling
                grown[exponent] -= coeffs[exponent] * other_time / scaling
            coeffs = grown
        for section in range(4):
            integrals[section, column] = sum(
                (
                    coeffs[exponent]
                    * (
                        node_times[section + 1] ** (exponent + 1)
                        - node_times[section] ** (exponent + 1)
                    )
                    / (exponent + 1)
                    for exponent in range(len(coeffs))
                )
            )
    coarse = [0.0, 0.5, 1.0]
    interp = np.zeros((5, 3))
    for column in range(3):
        for section in range(5):
            weight = 1.0
            for other_index in range(3):
                if other_index != column:
                    weight = (
                        weight
                        * (node_times[section] - coarse[other_index])
                        / (coarse[column] - coarse[other_index])
                    )
            interp[section, column] = weight
    return (np.array(node_times), integrals, interp)


def sine(length):
    k = np.arange(1, length + 1)
    phase = np.outer(k, k) % (2 * (length + 1))
    return math.sqrt(2.0 / (length + 1)) * np.sin(math.pi / (length + 1) * phase)


def eigen(length):
    return 2.0 - 2.0 * np.cos(math.pi / (length + 1) * np.arange(1, length + 1))


def split_pair(value):
    high = value.astype(jnp.bfloat16)
    return high, (value - high.astype(jnp.float32)).astype(jnp.bfloat16)


def dot(a, b):
    return jnp.dot(a, b, preferred_element_type=jnp.float32)


def along_y(field, w_ref):
    width = field.shape[1]
    both = dot(jnp.concatenate(split_pair(field), axis=1), w_ref[...])
    return both[:, :width] + both[:, width:]


def along_x(pair, high, x_ref, low_ref):
    return dot(x_ref[...], pair) + dot(low_ref[...], high)


def lateral(field, x_ref, low_ref, w_ref):
    depth, width_x, width_y = field.shape
    mixed = along_y(field.reshape(depth * width_x, width_y), w_ref)
    mixed = jnp.concatenate([mixed[z * width_x : (z + 1) * width_x] for z in range(depth)], axis=1)
    high, low = split_pair(mixed)
    out = along_x(jnp.concatenate([high, low], axis=0), high, x_ref, low_ref)
    return [out[:, z * width_y : (z + 1) * width_y] for z in range(depth)]


def z_sine(planes):
    count = len(planes)
    table = sine(count)
    half = (count + 1) // 2
    pairs = [
        (planes[z] + planes[count - 1 - z], planes[z] - planes[count - 1 - z])
        if z != count - 1 - z
        else (planes[z], None)
        for z in range(half)
    ]
    out = []
    for k in range(count):
        terms = [
            float(table[k, z]) * pairs[z][k % 2] for z in range(half) if pairs[z][k % 2] is not None
        ]
        total = terms[0]
        for term in terms[1:]:
            total = total + term
        out.append(total)
    return out


def weighted(weights, items):
    total = None
    for weight, item in zip(weights, items):
        weight = float(weight)
        if weight == 0.0 or item is None:
            continue
        term = item if weight == 1.0 else weight * item
        total = term if total is None else total + term
    return total


def sweep(rate, nodes, sources):
    times, integrals, _ = TABLES
    swept = [nodes[0]]
    for m in range(4):
        spacing = float(times[m + 1] - times[m])
        inner = weighted(integrals[m], nodes)
        if m > 0:
            inner = inner + spacing * (swept[m] - nodes[m])
        step = rate * inner
        if swept[m] is not None:
            step = step + swept[m]
        if sources is not None:
            step = step + sources[m]
        swept.append(step)
    first = list(integrals[0] + integrals[1])
    second = list(integrals[2] + integrals[3])
    first[0] -= 0.5
    second[2] -= 0.5
    left = rate * weighted(first, swept)
    right = rate * weighted(second, swept)
    if sources is not None:
        left = left + (sources[0] + sources[1])
        right = right + (sources[2] + sources[3])
    return swept, left, right


def corrected(swept, left, right, middle):
    interp = TABLES[2]
    ending = middle * left + right
    deltas = [None if swept[0] is None else -swept[0], left - swept[2], ending - swept[4]]
    return [
        None,
        swept[1] + weighted(interp[1], deltas),
        left,
        swept[3] + weighted(interp[3], deltas),
        ending,
    ]


def start_gains(middle):
    interp = TABLES[2]
    square = middle * middle
    return [
        None,
        float(interp[1, 0]) + float(interp[1, 1]) * middle + float(interp[1, 2]) * square,
        middle,
        float(interp[3, 0]) + float(interp[3, 1]) * middle + float(interp[3, 2]) * square,
        square,
    ]


def gains_of(rate):
    middle = 1.0 + 0.5 * rate
    gains = start_gains(middle)
    nodes = [jnp.ones_like(middle)] + gains[1:]
    swept, left, right = sweep(rate, nodes, None)
    return gains, corrected(swept, left, right, middle)


TABLES = node_tables()


def kernel(
    dims,
    step_ref, initial_hbm, guess_hbm, forcing_hbm, x_hbm, low_hbm, w_hbm, lateral_hbm,
    result_ref,
    initial, guess, forcing, x_ref, low_ref, w_ref, lateral_ref,
    in_send, in_recv, ghat, hhat, ell, own_step, steps,
    gain_c, gain_d, part_b, z_send, z_recv, own_gain, own_cross, r_send, r_recv,
    s_send, s_recv, o_send, o_recv, mix,
    load_sem, in_rs, h_rs, z_rs, s_rs, r_rs, o_rs, sent, signals,
):
    spaces, slices, chunks, depth, length_z, rows, width_y, group, block = dims
    me = lax.axis_index("space")
    place = lax.axis_index("tm")
    _, integrals, _ = TABLES
    width_x = spaces * chunks * rows
    everyone = spaces - 2
    last_group = slices // group - 1
    family, mine = place // group, lax.rem(place, group)
    eldest = place - mine
    near_sem, next_sem, open_sem = (signals.at[i] for i in range(3))
    in_ss, h_ss, step_ss, z_ss, s_ss, r_ss, o_ss, step_rs = (sent.at[i] for i in range(8))

    barrier = pltpu.get_barrier_semaphore()
    odd = lax.rem(me, 2) == 1
    for i in range(1, spaces):
        peer = lax.rem(me + i, spaces)

        @pl.when(lax.rem(peer, 2) == 1)
        def _():
            pl.semaphore_signal(barrier, inc=1, device_id={"space": peer}, device_id_type=MESH)

    sources = (
        guess_hbm.at[0], w_hbm, x_hbm, low_hbm, forcing_hbm.at[0], initial_hbm, lateral_hbm
    )
    loads = [
        pltpu.make_async_copy(source, target, load_sem.at[i])
        for i, (source, target) in enumerate(
            zip(sources, (guess, w_ref, x_ref, low_ref, forcing, initial, lateral_ref))
        )
    ]
    for load in loads:
        load.start()
    load_guess, load_w, load_x, load_low, load_forcing, load_initial, load_lateral = loads

    step = step_ref[0]
    own_step[...] = jnp.full(own_step.shape, step, jnp.float32)
    steps[mine] = jnp.full(own_step.shape, step, jnp.float32)

    def bulk(ref, sem):
        pltpu.make_async_copy(ref, ref, sem).wait()

    def low_of(c, s):
        return (c * spaces + s) * rows

    def put(field, slot):
        planes = lateral(field, x_ref, low_ref, w_ref)
        for target in range(spaces):
            for c in range(chunks):
                low = low_of(c, target)
                for z in range(depth):
                    in_send[c, target, slot, z] = planes[z][low : low + rows]

    def keep(c, low, high):
        in_recv[c, me, low:high] = in_send[c, me, low:high]

    def in_start(c, sem, low, high):
        for i in range(1, spaces):
            peer = lax.rem(me + i, spaces)
            pltpu.make_async_remote_copy(
                src_ref=in_send.at[c, peer, low:high],
                dst_ref=in_recv.at[c, me, low:high],
                send_sem=in_ss,
                recv_sem=in_rs.at[c, sem],
                device_id={"space": peer},
                device_id_type=MESH,
            ).start()

    def in_wait(c, sem, low, high):
        bulk(in_recv.at[c, 0 : spaces - 1, low:high], in_rs.at[c, sem])

    load_guess.wait()
    load_w.wait()
    load_x.wait()
    load_low.wait()
    put(guess[...], 0)

    @pl.when(odd)
    def _():
        pl.semaphore_wait(barrier, spaces - 1)
        pl.semaphore_signal(near_sem, inc=1, device_id={"space": me - 1}, device_id_type=MESH)

    @pl.when(jnp.logical_not(odd))
    def _():
        pl.semaphore_wait(near_sem, 1)

    for c in range(chunks):
        in_start(c, 0, 0, 1)

    @pl.when(jnp.logical_and(me == 0, place > 0))
    def _():
        pl.semaphore_signal(barrier, inc=1, device_id={"tm": place - 1}, device_id_type=MESH)

    def relatives(action):
        for i in range(1, group):
            action(lax.rem(mine + i, group))

    @pl.when(me == everyone)
    def _():
        def greet(target):
            pl.semaphore_signal(barrier, inc=1, device_id={"tm": target}, device_id_type=MESH)

        relatives(lambda other: greet(eldest + other))
        pl.when(family > 0)(lambda: greet(place - group))

    def tell(sem):
        for i in range(1, spaces):
            pl.semaphore_signal(
                sem, inc=1, device_id={"space": lax.rem(me + i, spaces)}, device_id_type=MESH
            )

    for c in range(chunks):
        keep(c, 0, 1)
    load_forcing.wait()
    for m in range(4):
        put(step * weighted(integrals[m], [forcing[j] for j in range(5)]), m + 1)

    load_initial.wait()

    @pl.when(place == 0)
    def _():
        put(initial[...], 5)
        for c in range(chunks):
            in_start(c, 1, 1, 6)

    @pl.when(place > 0)
    def _():
        for c in range(chunks):
            in_start(c, 1, 1, 5)

    for c in range(chunks):
        keep(c, 1, 5)

        @pl.when(place == 0)
        def _():
            keep(c, 5, 6)

    z_eigen = eigen(length_z)
    load_lateral.wait()
    for c in range(chunks):
        low = pl.multiple_of(low_of(c, me), 8)
        base = lateral_ref[pl.ds(low, rows), :]
        for k in range(length_z):
            ell[c, k * rows : (k + 1) * rows] = -(base + float(z_eigen[k]))

    def table(i, carry):
        for c in range(chunks):
            at = pl.ds(pl.multiple_of(i * rows, 8), rows)
            gains, crossed = gains_of(step * ell[c, at])
            for m in range(1, 5):
                gain_c[c, m - 1, at] = gains[m]
                gain_d[c, m - 1, at] = crossed[m]
        return carry

    lax.fori_loop(0, length_z, table, 0)

    def planes_of(c, slot):
        return [in_recv[c, z // depth, slot, z % depth] for z in range(length_z)]

    @pl.when(place < slices - 1)
    def _():
        @pl.when(me == 0)
        def _():
            pl.semaphore_wait(barrier, 1)
            tell(next_sem)

        @pl.when(me != 0)
        def _():
            pl.semaphore_wait(next_sem, 1)

    after = lax.rem(place + 1, slices)
    for c in range(chunks):
        in_wait(c, 0, 0, 1)
        for k, plane in enumerate(z_sine(planes_of(c, 0))):
            ghat[c, k * rows : (k + 1) * rows] = plane

        @pl.when(place < slices - 1)
        def _():
            pltpu.make_async_remote_copy(
                src_ref=ghat.at[c],
                dst_ref=hhat.at[c],
                send_sem=h_ss,
                recv_sem=h_rs.at[c],
                device_id={"tm": after},
                device_id_type=MESH,
            ).start()

    def opened():
        @pl.when(me == everyone)
        def _():
            pl.when(family < last_group)(lambda: pl.semaphore_wait(barrier, group))
            pl.when(family == last_group)(lambda: pl.semaphore_wait(barrier, group - 1))
            tell(open_sem)

        @pl.when(me != everyone)
        def _():
            pl.semaphore_wait(open_sem, 1)

        relatives(
            lambda other: pltpu.make_async_remote_copy(
                src_ref=own_step,
                dst_ref=steps.at[mine],
                send_sem=step_ss,
                recv_sem=step_rs,
                device_id={"tm": eldest + other},
                device_id_type=MESH,
            ).start()
        )

    def z_start(c):
        relatives(
            lambda other: pltpu.make_async_remote_copy(
                src_ref=z_send.at[c, other],
                dst_ref=z_recv.at[c, mine],
                send_sem=z_ss,
                recv_sem=z_rs.at[c],
                device_id={"tm": eldest + other},
                device_id_type=MESH,
            ).start()
        )

    first = jnp.where(place == 0, 1.0, 0.0).astype(jnp.float32)
    for c in range(chunks):
        @pl.when(place == 0)
        def _():
            in_wait(c, 1, 1, 6)
            for k, plane in enumerate(z_sine(planes_of(c, 5))):
                hhat[c, k * rows : (k + 1) * rows] = plane

        @pl.when(place > 0)
        def _():
            in_wait(c, 1, 1, 5)
            bulk(hhat.at[c], h_rs.at[c])

        fhat = [z_sine(planes_of(c, m + 1)) for m in range(4)]
        for m in range(4):
            for k in range(length_z):
                part_b[c, m, k * rows : (k + 1) * rows] = fhat[m][k]

        def solve(i, carry):
            at = pl.ds(pl.multiple_of(i * block, 8), block)
            rate = step * ell[c, at]
            middle = 1.0 + 0.5 * rate
            guess_hat, start = ghat[c, at], hhat[c, at]
            sources = [part_b[c, m, at] for m in range(4)]
            one = sweep(rate, [start] + [guess_hat] * 4, sources)
            nodes = corrected(*one, middle)
            rest = corrected(*sweep(rate, nodes, sources), middle)
            for m in range(1, 5):
                part_b[c, m - 1, at] = rest[m]
            seen = first * start
            gain, cross = gain_c[c, 3, at], gain_d[c, 3, at]
            z_send[c, i, 0] = nodes[4] + gain * seen
            z_send[c, i, 1] = rest[4] + (gain + cross) * seen
            return carry

        lax.fori_loop(0, group, solve, 0, unroll=4)
        if c == 0:
            opened()

        pl.when(place < slices - 1)(lambda: z_start(c))
        z_recv[c, mine] = z_send[c, mine]

    bulk(steps.at[0 : group - 1], step_rs)
    at = pl.ds(pl.multiple_of(mine * block, 8), block)

    def one(p, carry):
        for c in range(chunks):
            gains, crossed = gains_of(steps[p][0:1] * ell[c, at])
            own_gain[c, p] = gains[4]
            own_cross[c, p] = crossed[4]
        return carry

    lax.fori_loop(0, group, one, 0)

    def r_start(c, other):
        pltpu.make_async_remote_copy(
            src_ref=r_send.at[c, other],
            dst_ref=r_recv.at[c, mine],
            send_sem=r_ss,
            recv_sem=r_rs.at[c],
            device_id={"tm": eldest + other},
            device_id_type=MESH,
        ).start()

    short = jnp.logical_and(family == last_group, place < slices - 1)
    for c in range(chunks):
        if group > 2:
            pl.when(short)(lambda: bulk(z_recv.at[c, 0 : group - 2], z_rs.at[c]))
        pl.when(jnp.logical_not(short))(lambda: bulk(z_recv.at[c, 0 : group - 1], z_rs.at[c]))
        pl.when(family > 0)(lambda: bulk(s_recv.at[c], s_rs.at[c]))

        def advance(p, lower, upper):
            gain = own_gain[c, p]
            return (
                gain * lower + z_recv[c, p, 0],
                gain * upper + own_cross[c, p] * lower + z_recv[c, p, 1],
            )

        lower, upper = (jnp.where(family > 0, s_recv[c, i], 0.0) for i in range(2))
        for p in range(group):
            r_send[c, p, 0] = lower
            r_send[c, p, 1] = upper
            if p < group - 1:
                lower, upper = advance(p, lower, upper)

        @pl.when(family < last_group)
        def _():
            final = advance(group - 1, lower, upper)
            s_send[c, 0], s_send[c, 1] = final
            pltpu.make_async_remote_copy(
                src_ref=s_send.at[c],
                dst_ref=s_recv.at[c],
                send_sem=s_ss,
                recv_sem=s_rs.at[c],
                device_id={"tm": place + group},
                device_id_type=MESH,
            ).start()

        relatives(lambda other: pl.when(eldest + other > 0)(lambda: r_start(c, other)))
        r_recv[c, mine] = r_send[c, mine]

    halves = ((0, 3), (3, 5))

    def o_groups(c):
        return halves if c == chunks - 1 else ((0, 5),)

    def o_start(c, number):
        low, high = o_groups(c)[number]
        for i in range(1, spaces):
            peer = lax.rem(me + i, spaces)
            pltpu.make_async_remote_copy(
                src_ref=o_send.at[c, peer, low:high],
                dst_ref=o_recv.at[c, me, low:high],
                send_sem=o_ss,
                recv_sem=o_rs.at[c + number],
                device_id={"space": peer},
                device_id_type=MESH,
            ).start()

    def o_wait(c, number):
        low, high = o_groups(c)[number]
        bulk(o_recv.at[c, 0 : spaces - 1, low:high], o_rs.at[c + number])

    for c in range(chunks):
        pl.when(place > 0)(lambda: bulk(r_recv.at[c, 0 : group - 1], r_rs.at[c]))
        own = hhat[c].reshape(group, block, width_y)
        lower = jnp.where(place == 0, own, r_recv[c, :, 0]).reshape(length_z * rows, width_y)
        upper = jnp.where(place == 0, own, r_recv[c, :, 1]).reshape(length_z * rows, width_y)
        for m in range(5):
            if m == 0:
                value = upper
            else:
                value = (
                    gain_c[c, m - 1] * upper + gain_d[c, m - 1] * lower + part_b[c, m - 1]
                )
            planes = z_sine([value[k * rows : (k + 1) * rows] for k in range(length_z)])
            for z in range(length_z):
                o_send[c, z // depth, m, z % depth] = planes[z]
            for number, (_, high) in enumerate(o_groups(c)):
                if high == m + 1:
                    o_start(c, number)
            o_recv[c, me, m] = o_send[c, me, m]

    def unmix(c, low, high):
        stacked = jnp.concatenate(
            [
                o_recv[c, s, m, z]
                for m in range(low, high)
                for z in range(depth)
                for s in range(spaces)
            ],
            axis=0,
        )
        tall = spaces * rows
        mixed_high, mixed_low = split_pair(along_y(stacked, w_ref))
        for m in range(low, high):
            for z in range(depth):
                at = ((m - low) * depth + z) * tall
                lanes = slice(z * width_y, (z + 1) * width_y)
                mix[m, c * tall : (c + 1) * tall, lanes] = mixed_high[at : at + tall]
                mix[m, width_x + c * tall : width_x + (c + 1) * tall, lanes] = mixed_low[
                    at : at + tall
                ]

    for c in range(chunks - 1):
        o_wait(c, 0)
        unmix(c, 0, 5)
    for number, (low, high) in enumerate(halves):
        o_wait(chunks - 1, number)
        unmix(chunks - 1, low, high)
        for m in range(low, high):
            out = along_x(mix[m], mix[m, :width_x], x_ref, low_ref)
            for z in range(depth):
                result_ref[0, m, z] = out[:, z * width_y : (z + 1) * width_y]

    others = spaces - 1
    pl.when(place == 0)(lambda: bulk(in_send.at[:, 0:others], in_ss))
    pl.when(place > 0)(lambda: bulk(in_send.at[:, 0:others, 0:5], in_ss))
    bulk(o_send.at[:, 0:others], o_ss)
    bulk(steps.at[0 : group - 1], step_ss)

    @pl.when(place < slices - 1)
    def _():
        bulk(ghat, h_ss)
        bulk(z_send.at[:, 0 : group - 1], z_ss)

    pl.when(family < last_group)(lambda: bulk(s_send, s_ss))
    fewer = jnp.logical_and(family == 0, place > 0)
    if group > 2:
        pl.when(fewer)(lambda: bulk(r_send.at[:, 0 : group - 2], r_ss))
    pl.when(jnp.logical_not(fewer))(lambda: bulk(r_send.at[:, 0 : group - 1], r_ss))


def body(initial, start_guess, forcing, step_size):
    depth, width_x, width_y = initial.shape
    spaces, slices = lax.axis_size("space"), lax.axis_size("tm")
    length_z = depth * spaces
    chunks = CHUNKS
    rows = width_x // spaces // chunks
    group = max(1, min(GROUP, slices // 2))
    block = length_z * rows // group
    dims = (spaces, slices, chunks, depth, length_z, rows, width_y, group, block)

    def pair(length):
        return split_pair(jnp.asarray(sine(length), jnp.float32))

    x_high, x_low = pair(width_x)
    y_high, y_low = pair(width_y)
    x_twice = jnp.concatenate([x_high, x_high], axis=1)
    w = jnp.concatenate(
        [
            jnp.concatenate([y_high, y_low], axis=1),
            jnp.concatenate([y_high, jnp.zeros_like(y_low)], axis=1),
        ],
        axis=0,
    )
    sides = jnp.asarray(eigen(width_x)[:, None] + eigen(width_y)[None, :], jnp.float32)
    f32, b16 = jnp.float32, jnp.bfloat16
    flat = length_z * rows
    dma = pltpu.SemaphoreType.DMA
    vmem = pl.BlockSpec(memory_space=pltpu.VMEM)
    hbm = pl.BlockSpec(memory_space=pl.ANY)
    return pl.pallas_call(
        functools.partial(kernel, dims),
        out_shape=pltpu.VMEM((1, 5, depth, width_x, width_y), f32),
        in_specs=[pl.BlockSpec(memory_space=pltpu.SMEM)] + [hbm] * 7,
        out_specs=vmem,
        scratch_shapes=[
            pltpu.VMEM((depth, width_x, width_y), f32),
            pltpu.VMEM((depth, width_x, width_y), f32),
            pltpu.VMEM((5, depth, width_x, width_y), f32),
            pltpu.VMEM((width_x, 2 * width_x), b16),
            pltpu.VMEM((width_x, width_x), b16),
            pltpu.VMEM((2 * width_y, 2 * width_y), b16),
            pltpu.VMEM((width_x, width_y), f32),
            pltpu.VMEM((chunks, spaces, 6, depth, rows, width_y), f32),
            pltpu.VMEM((chunks, spaces, 6, depth, rows, width_y), f32),
            pltpu.VMEM((chunks, flat, width_y), f32),
            pltpu.VMEM((chunks, flat, width_y), f32),
            pltpu.VMEM((chunks, flat, width_y), f32),
            pltpu.VMEM((8, width_y), f32),
            pltpu.VMEM((group, 8, width_y), f32),
            pltpu.VMEM((chunks, 4, flat, width_y), f32),
            pltpu.VMEM((chunks, 4, flat, width_y), f32),
            pltpu.VMEM((chunks, 4, flat, width_y), f32),
            pltpu.VMEM((chunks, group, 2, block, width_y), f32),
            pltpu.VMEM((chunks, group, 2, block, width_y), f32),
            pltpu.VMEM((chunks, group, block, width_y), f32),
            pltpu.VMEM((chunks, group, block, width_y), f32),
            pltpu.VMEM((chunks, group, 2, block, width_y), f32),
            pltpu.VMEM((chunks, group, 2, block, width_y), f32),
            pltpu.VMEM((chunks, 2, block, width_y), f32),
            pltpu.VMEM((chunks, 2, block, width_y), f32),
            pltpu.VMEM((chunks, spaces, 5, depth, rows, width_y), f32),
            pltpu.VMEM((chunks, spaces, 5, depth, rows, width_y), f32),
            pltpu.VMEM((5, 2 * width_x, depth * width_y), b16),
            dma((7,)),
            dma((chunks, 2)),
            dma((chunks,)),
            dma((chunks,)),
            dma((chunks,)),
            dma((chunks,)),
            dma((chunks + 1,)),
            dma((8,)),
            pltpu.SemaphoreType.REGULAR((3,)),
        ],
        compiler_params=pltpu.CompilerParams(collective_id=0, has_side_effects=True),
    )(step_size, initial, start_guess, forcing, x_twice, x_low, w, sides)


def solution(mesh):
    in_specs = (
        P("space", None, None),
        P("tm", "space", None, None),
        P("tm", None, "space", None, None),
        P("tm"),
    )
    out_specs = P("tm", None, "space", None, None)
    return jax.shard_map(body, mesh=mesh, in_specs=in_specs, out_specs=out_specs, check_vma=False)
```

```python
import functools
import math

import jax
import jax.numpy as jnp
import numpy as np
from jax import lax
from jax.experimental import pallas as pl
from jax.experimental.pallas import tpu as pltpu
from jax.sharding import PartitionSpec as P

MESH = pl.DeviceIdType.MESH
CHUNKS = 4
GROUP = 8

def node_tables():
    radical = math.sqrt(3.0 / 7.0)
    node_times = [0.0, (1.0 - radical) / 2.0, 0.5, (1.0 + radical) / 2.0, 1.0]
    integrals = np.zeros((4, 5))
    for column in range(5):
        coeffs = [1.0]
        for other_index in range(5):
            if other_index == column:
                continue
            other_time = node_times[other_index]
            scaling = node_times[column] - other_time
            grown = [0.0] * (len(coeffs) + 1)
            for exponent in range(len(coeffs)):
                grown[exponent + 1] += coeffs[exponent] / scaling
                grown[exponent] -= coeffs[exponent] * other_time / scaling
            coeffs = grown
        for section in range(4):
            integrals[section, column] = sum(
                (
                    coeffs[exponent]
                    * (
                        node_times[section + 1] ** (exponent + 1)
                        - node_times[section] ** (exponent + 1)
                    )
                    / (exponent + 1)
                    for exponent in range(len(coeffs))
                )
            )
    coarse = [0.0, 0.5, 1.0]
    interp = np.zeros((5, 3))
    for column in range(3):
        for section in range(5):
            weight = 1.0
            for other_index in range(3):
                if other_index != column:
                    weight = (
                        weight
                        * (node_times[section] - coarse[other_index])
                        / (coarse[column] - coarse[other_index])
                    )
            interp[section, column] = weight
    return (np.array(node_times), integrals, interp)


def sine(length):
    k = np.arange(1, length + 1)
    phase = np.outer(k, k) % (2 * (length + 1))
    return math.sqrt(2.0 / (length + 1)) * np.sin(math.pi / (length + 1) * phase)


def eigen(length):
    return 2.0 - 2.0 * np.cos(math.pi / (length + 1) * np.arange(1, length + 1))


def split_pair(value):
    high = value.astype(jnp.bfloat16)
    return high, (value - high.astype(jnp.float32)).astype(jnp.bfloat16)


def dot(a, b):
    return jnp.dot(a, b, preferred_element_type=jnp.float32)


def along_y(field, w_ref):
    width = field.shape[1]
    both = dot(jnp.concatenate(split_pair(field), axis=1), w_ref[...])
    return both[:, :width] + both[:, width:]


def along_x(pair, high, x_ref, low_ref):
    return dot(x_ref[...], pair) + dot(low_ref[...], high)


def lateral(field, x_ref, low_ref, w_ref):
    depth, width_x, width_y = field.shape
    mixed = along_y(field.reshape(depth * width_x, width_y), w_ref)
    mixed = jnp.concatenate([mixed[z * width_x : (z + 1) * width_x] for z in range(depth)], axis=1)
    high, low = split_pair(mixed)
    out = along_x(jnp.concatenate([high, low], axis=0), high, x_ref, low_ref)
    return [out[:, z * width_y : (z + 1) * width_y] for z in range(depth)]


def z_sine(planes):
    count = len(planes)
    table = sine(count)
    half = (count + 1) // 2
    pairs = [
        (planes[z] + planes[count - 1 - z], planes[z] - planes[count - 1 - z])
        if z != count - 1 - z
        else (planes[z], None)
        for z in range(half)
    ]
    out = []
    for k in range(count):
        terms = [
            float(table[k, z]) * pairs[z][k % 2] for z in range(half) if pairs[z][k % 2] is not None
        ]
        total = terms[0]
        for term in terms[1:]:
            total = total + term
        out.append(total)
    return out


def weighted(weights, items):
    total = None
    for weight, item in zip(weights, items):
        weight = float(weight)
        if weight == 0.0 or item is None:
            continue
        term = item if weight == 1.0 else weight * item
        total = term if total is None else total + term
    return total


def sweep(rate, nodes, sources):
    times, integrals, _ = TABLES
    swept = [nodes[0]]
    for m in range(4):
        spacing = float(times[m + 1] - times[m])
        inner = weighted(integrals[m], nodes)
        if m > 0:
            inner = inner + spacing * (swept[m] - nodes[m])
        step = rate * inner
        if swept[m] is not None:
            step = step + swept[m]
        if sources is not None:
            step = step + sources[m]
        swept.append(step)
    first = list(integrals[0] + integrals[1])
    second = list(integrals[2] + integrals[3])
    first[0] -= 0.5
    second[2] -= 0.5
    left = rate * weighted(first, swept)
    right = rate * weighted(second, swept)
    if sources is not None:
        left = left + (sources[0] + sources[1])
        right = right + (sources[2] + sources[3])
    return swept, left, right


def corrected(swept, left, right, middle):
    interp = TABLES[2]
    ending = middle * left + right
    deltas = [None if swept[0] is None else -swept[0], left - swept[2], ending - swept[4]]
    return [
        None,
        swept[1] + weighted(interp[1], deltas),
        left,
        swept[3] + weighted(interp[3], deltas),
        ending,
    ]


def start_gains(middle):
    interp = TABLES[2]
    square = middle * middle
    return [
        None,
        float(interp[1, 0]) + float(interp[1, 1]) * middle + float(interp[1, 2]) * square,
        middle,
        float(interp[3, 0]) + float(interp[3, 1]) * middle + float(interp[3, 2]) * square,
        square,
    ]


def gains_of(rate):
    middle = 1.0 + 0.5 * rate
    gains = start_gains(middle)
    nodes = [jnp.ones_like(middle)] + gains[1:]
    swept, left, right = sweep(rate, nodes, None)
    return gains, corrected(swept, left, right, middle)


TABLES = node_tables()


def kernel(
    dims,
    step_ref, initial_hbm, guess_hbm, forcing_hbm, x_hbm, low_hbm, w_hbm, lateral_hbm,
    result_ref,
    initial, guess, forcing, x_ref, low_ref, w_ref, lateral_ref,
    in_send, in_recv, ghat, hhat, ell, own_step, steps,
    first_hat, gain_c, gain_d, part_b, z_send, z_recv, own_gain, own_cross, r_send, r_recv,
    s_send, s_recv, o_send, o_recv, mix,
    load_sem, in_rs, h_rs, z_rs, s_rs, r_rs, o_rs, sent, signals,
):
    spaces, slices, chunks, depth, length_z, rows, width_y, group, block = dims
    me = lax.axis_index("space")
    place = lax.axis_index("tm")
    _, integrals, _ = TABLES
    width_x = spaces * chunks * rows
    everyone = spaces - 2
    last_group = slices // group - 1
    family, mine = place // group, lax.rem(place, group)
    eldest = place - mine
    near_sem, next_sem, open_sem = (signals.at[i] for i in range(3))
    h_ss, step_ss, z_ss, s_ss, r_ss, o_ss, step_rs = (sent.at[i] for i in range(7))
    in_ss = [sent.at[7 + i] for i in range(4)]
    first_in_ss, first_in_rs, first_ss = (sent.at[11 + i] for i in range(3))
    helper = jnp.logical_and(family == 0, mine < chunks)

    barrier = pltpu.get_barrier_semaphore()
    odd = lax.rem(me, 2) == 1
    for i in range(1, spaces):
        peer = lax.rem(me + i, spaces)

        @pl.when(lax.rem(peer, 2) == 1)
        def _():
            pl.semaphore_signal(barrier, inc=1, device_id={"space": peer}, device_id_type=MESH)

    sources = (
        guess_hbm.at[0], w_hbm, x_hbm, low_hbm, forcing_hbm.at[0], initial_hbm, lateral_hbm
    )
    loads = [
        pltpu.make_async_copy(source, target, load_sem.at[i])
        for i, (source, target) in enumerate(
            zip(sources, (guess, w_ref, x_ref, low_ref, forcing, initial, lateral_ref))
        )
    ]
    for load in loads:
        load.start()
    load_guess, load_w, load_x, load_low, load_forcing, load_initial, load_lateral = loads

    step = step_ref[0]
    own_step[...] = jnp.full(own_step.shape, step, jnp.float32)
    steps[mine] = jnp.full(own_step.shape, step, jnp.float32)

    def bulk(ref, sem):
        pltpu.make_async_copy(ref, ref, sem).wait()

    def low_of(c, s):
        return (c * spaces + s) * rows

    def put(field, slot):
        planes = lateral(field, x_ref, low_ref, w_ref)
        for target in range(spaces):
            for c in range(chunks):
                low = low_of(c, target)
                for z in range(depth):
                    in_send[c, target, slot, z] = planes[z][low : low + rows]

    def keep(c, low, high):
        in_recv[c, me, low:high] = in_send[c, me, low:high]

    def in_start(c, low, high, left, landed):
        for i in range(1, spaces):
            peer = lax.rem(me + i, spaces)
            pltpu.make_async_remote_copy(
                src_ref=in_send.at[c, peer, low:high],
                dst_ref=in_recv.at[c, me, low:high],
                send_sem=left,
                recv_sem=landed,
                device_id={"space": peer},
                device_id_type=MESH,
            ).start()

    def in_wait(c, low, high, landed):
        bulk(in_recv.at[c, 0 : spaces - 1, low:high], landed)

    load_guess.wait()
    load_w.wait()
    load_x.wait()
    load_low.wait()
    put(guess[...], 0)

    @pl.when(odd)
    def _():
        pl.semaphore_wait(barrier, spaces - 1)
        pl.semaphore_signal(near_sem, inc=1, device_id={"space": me - 1}, device_id_type=MESH)

    @pl.when(jnp.logical_not(odd))
    def _():
        pl.semaphore_wait(near_sem, 1)

    def guess_start(c):
        in_start(c, 0, 1, in_ss[0], in_rs.at[c, 0])

    for c in range(chunks // 2):
        guess_start(c)

    def greet(target):
        pl.semaphore_signal(barrier, inc=1, device_id={"tm": target}, device_id_type=MESH)

    @pl.when(me == 0)
    def _():
        pl.when(place > 0)(lambda: greet(place - 1))

        @pl.when(place == 0)
        def _():
            for other in range(1, min(chunks, group)):
                greet(other)

    def relatives(action):
        for i in range(1, group):
            action(lax.rem(mine + i, group))

    @pl.when(me == everyone)
    def _():
        relatives(lambda other: greet(eldest + other))
        pl.when(family > 0)(lambda: greet(place - group))

    def tell(sem):
        for i in range(1, spaces):
            pl.semaphore_signal(
                sem, inc=1, device_id={"space": lax.rem(me + i, spaces)}, device_id_type=MESH
            )

    load_initial.wait()

    @pl.when(helper)
    def _():
        put(initial[...], 5)
        in_start(mine, 5, 6, first_in_ss, first_in_rs)
        keep(mine, 5, 6)

    for c in range(chunks // 2, chunks):
        guess_start(c)
    for c in range(chunks):
        keep(c, 0, 1)
    load_forcing.wait()
    for m in range(4):
        put(step * weighted(integrals[m], [forcing[j] for j in range(5)]), m + 1)

    last_left = 3

    def forcing_start(c):
        in_start(c, 1, 5, in_ss[min(c + 1, last_left)], in_rs.at[c, 1])

    def forcing_left(c):
        bulk(in_send.at[c, 0 : spaces - 1, 1:5], in_ss[c + 1])

    forcing_start(0)

    for c in range(chunks):
        keep(c, 1, 5)

    z_eigen = eigen(length_z)
    load_lateral.wait()
    for c in range(chunks):
        low = pl.multiple_of(low_of(c, me), 8)
        base = lateral_ref[pl.ds(low, rows), :]
        for k in range(length_z):
            ell[c, k * rows : (k + 1) * rows] = -(base + float(z_eigen[k]))

    def table(i, carry):
        for c in range(chunks):
            at = pl.ds(pl.multiple_of(i * rows, 8), rows)
            gains, crossed = gains_of(step * ell[c, at])
            for m in range(1, 5):
                gain_c[c, m - 1, at] = gains[m]
                gain_d[c, m - 1, at] = crossed[m]
        return carry

    lax.fori_loop(0, length_z, table, 0)

    def planes_of(c, slot):
        return [in_recv[c, z // depth, slot, z % depth] for z in range(length_z)]

    helping = jnp.logical_and(helper, place > 0)
    hands = jnp.logical_or(helping, place < slices - 1)

    @pl.when(me == 0)
    def _():
        both = jnp.logical_and(helping, place < slices - 1)
        pl.when(both)(lambda: pl.semaphore_wait(barrier, 2))
        pl.when(jnp.logical_and(hands, jnp.logical_not(both)))(
            lambda: pl.semaphore_wait(barrier, 1)
        )
        pl.when(hands)(lambda: tell(next_sem))

    bulk(in_send.at[:, 0 : spaces - 1, 0:1], in_ss[0])
    if chunks > 1:
        forcing_start(1)

    pl.when(jnp.logical_and(hands, me != 0))(lambda: pl.semaphore_wait(next_sem, 1))
    after = lax.rem(place + 1, slices)
    def hand(source, target, c, left):
        pltpu.make_async_remote_copy(
            src_ref=source,
            dst_ref=hhat.at[c],
            send_sem=left,
            recv_sem=h_rs.at[c],
            device_id={"tm": target},
            device_id_type=MESH,
        ).start()

    def hand_guess(c):
        in_wait(c, 0, 1, in_rs.at[c, 0])
        for k, plane in enumerate(z_sine(planes_of(c, 0))):
            ghat[c, k * rows : (k + 1) * rows] = plane
        pl.when(place < slices - 1)(lambda: hand(ghat.at[c], after, c, h_ss))

    for c in range(chunks // 2):
        hand_guess(c)

    @pl.when(helper)
    def _():
        in_wait(mine, 5, 6, first_in_rs)
        for k, plane in enumerate(z_sine(planes_of(mine, 5))):
            first_hat[k * rows : (k + 1) * rows] = plane

        @pl.when(place == 0)
        def _():
            hhat[0] = first_hat[...]

        pl.when(place > 0)(lambda: hand(first_hat, 0, mine, first_ss))

    for c in range(chunks // 2, chunks):
        hand_guess(c)
    for c in range(2, chunks):
        if c < last_left + 1:
            forcing_left(c - 2)
        forcing_start(c)

        if c == 2:
            @pl.when(me == everyone)
            def _():
                pl.when(family < last_group)(lambda: pl.semaphore_wait(barrier, group))
                pl.when(family == last_group)(lambda: pl.semaphore_wait(barrier, group - 1))
                tell(open_sem)

    pl.when(me != everyone)(lambda: pl.semaphore_wait(open_sem, 1))
    relatives(
        lambda other: pltpu.make_async_remote_copy(
            src_ref=own_step,
            dst_ref=steps.at[mine],
            send_sem=step_ss,
            recv_sem=step_rs,
            device_id={"tm": eldest + other},
            device_id_type=MESH,
        ).start()
    )

    youngest = jnp.where(mine == group - 1, 1, 0)

    def z_start(c):
        relatives(
            lambda other: pltpu.make_async_remote_copy(
                src_ref=z_send.at[c, other],
                dst_ref=z_recv.at[c, mine],
                send_sem=z_ss,
                recv_sem=z_rs.at[c, youngest],
                device_id={"tm": eldest + other},
                device_id_type=MESH,
            ).start()
        )

    first = jnp.where(place == 0, 1.0, 0.0).astype(jnp.float32)

    def chunk(c):
        in_wait(c, 1, 5, in_rs.at[c, 1])
        if c == 0:
            pl.when(place > 0)(lambda: bulk(hhat.at[c], h_rs.at[c]))
        else:
            bulk(hhat.at[c], h_rs.at[c])
        fhat = [z_sine(planes_of(c, m + 1)) for m in range(4)]
        for m in range(4):
            for k in range(length_z):
                part_b[c, m, k * rows : (k + 1) * rows] = fhat[m][k]

        def solve(i, carry):
            at = pl.ds(pl.multiple_of(i * block, 8), block)
            rate = step * ell[c, at]
            middle = 1.0 + 0.5 * rate
            guess_hat, start = ghat[c, at], hhat[c, at]
            sources = [part_b[c, m, at] for m in range(4)]
            one = sweep(rate, [start] + [guess_hat] * 4, sources)
            nodes = corrected(*one, middle)
            rest = corrected(*sweep(rate, nodes, sources), middle)
            for m in range(1, 5):
                part_b[c, m - 1, at] = rest[m]
            seen = first * start
            gain, cross = gain_c[c, 3, at], gain_d[c, 3, at]
            z_send[c, i, 0] = nodes[4] + gain * seen
            z_send[c, i, 1] = rest[4] + (gain + cross) * seen
            return carry

        lax.fori_loop(0, group, solve, 0, unroll=4)
        pl.when(place < slices - 1)(lambda: z_start(c))
        z_recv[c, mine] = z_send[c, mine]

    at = pl.ds(pl.multiple_of(mine * block, 8), block)

    def own_tables():
        bulk(steps.at[0 : group - 1], step_rs)

        def one(p, carry):
            for c in range(chunks):
                gains, crossed = gains_of(steps[p][0:1] * ell[c, at])
                own_gain[c, p] = gains[4]
                own_cross[c, p] = crossed[4]
            return carry

        lax.fori_loop(0, group, one, 0)

    def r_start(c, other):
        pltpu.make_async_remote_copy(
            src_ref=r_send.at[c, other],
            dst_ref=r_recv.at[c, mine],
            send_sem=r_ss,
            recv_sem=r_rs.at[c],
            device_id={"tm": eldest + other},
            device_id_type=MESH,
        ).start()

    def scan(c):
        @pl.when(mine < group - 1)
        def _():
            if group > 2:
                bulk(z_recv.at[c, 0 : group - 2], z_rs.at[c, 0])

        pl.when(mine == group - 1)(lambda: bulk(z_recv.at[c, 0 : group - 1], z_rs.at[c, 0]))
        pl.when(family > 0)(lambda: bulk(s_recv.at[c], s_rs.at[c]))

        def advance(p, lower, upper):
            gain = own_gain[c, p]
            return (
                gain * lower + z_recv[c, p, 0],
                gain * upper + own_cross[c, p] * lower + z_recv[c, p, 1],
            )

        lower, upper = (jnp.where(family > 0, s_recv[c, i], 0.0) for i in range(2))
        for p in range(group):
            r_send[c, p, 0] = lower
            r_send[c, p, 1] = upper
            if p < group - 1:
                lower, upper = advance(p, lower, upper)

        relatives(lambda other: pl.when(eldest + other > 0)(lambda: r_start(c, other)))
        r_recv[c, mine] = r_send[c, mine]

        @pl.when(family < last_group)
        def _():
            pl.when(mine < group - 1)(lambda: bulk(z_recv.at[c, 0], z_rs.at[c, 1]))
            final = advance(group - 1, r_send[c, group - 1, 0], r_send[c, group - 1, 1])
            s_send[c, 0], s_send[c, 1] = final
            pltpu.make_async_remote_copy(
                src_ref=s_send.at[c],
                dst_ref=s_recv.at[c],
                send_sem=s_ss,
                recv_sem=s_rs.at[c],
                device_id={"tm": place + group},
                device_id_type=MESH,
            ).start()

    halves = ((0, 3), (3, 5))

    def o_groups(c):
        return halves if c == chunks - 1 else ((0, 5),)

    def o_start(c, number):
        low, high = o_groups(c)[number]
        for i in range(1, spaces):
            peer = lax.rem(me + i, spaces)
            pltpu.make_async_remote_copy(
                src_ref=o_send.at[c, peer, low:high],
                dst_ref=o_recv.at[c, me, low:high],
                send_sem=o_ss,
                recv_sem=o_rs.at[c + number],
                device_id={"space": peer},
                device_id_type=MESH,
            ).start()

    def o_wait(c, number):
        low, high = o_groups(c)[number]
        bulk(o_recv.at[c, 0 : spaces - 1, low:high], o_rs.at[c + number])

    def give(c, lower, upper):
        for m in range(5):
            if m == 0:
                value = upper
            else:
                value = (
                    gain_c[c, m - 1] * upper + gain_d[c, m - 1] * lower + part_b[c, m - 1]
                )
            planes = z_sine([value[k * rows : (k + 1) * rows] for k in range(length_z)])
            for z in range(length_z):
                o_send[c, z // depth, m, z % depth] = planes[z]
            for number, (_, high) in enumerate(o_groups(c)):
                if high == m + 1:
                    o_start(c, number)
            o_recv[c, me, m] = o_send[c, me, m]

    def give_first(c):
        own = hhat[c]
        give(c, own, own)

    def give_later(c):
        bulk(r_recv.at[c, 0 : group - 1], r_rs.at[c])
        give(c, *(r_recv[c, :, i].reshape(length_z * rows, width_y) for i in range(2)))

    for c in range(chunks - 1):
        chunk(c)
    own_tables()

    @pl.when(place == 0)
    def _():
        scan(0)
        chunk(chunks - 1)
        for c in range(1, chunks):
            scan(c)
            give_first(c - 1)
        give_first(chunks - 1)

    @pl.when(place > 0)
    def _():
        chunk(chunks - 1)
        for c in range(chunks):
            scan(c)
            if c >= 2:
                give_later(c - 2)
        for c in range(max(0, chunks - 2), chunks):
            give_later(c)

    def unmix(c, low, high):
        stacked = jnp.concatenate(
            [
                o_recv[c, s, m, z]
                for m in range(low, high)
                for z in range(depth)
                for s in range(spaces)
            ],
            axis=0,
        )
        tall = spaces * rows
        mixed_high, mixed_low = split_pair(along_y(stacked, w_ref))
        for m in range(low, high):
            for z in range(depth):
                at = ((m - low) * depth + z) * tall
                lanes = slice(z * width_y, (z + 1) * width_y)
                mix[m, c * tall : (c + 1) * tall, lanes] = mixed_high[at : at + tall]
                mix[m, width_x + c * tall : width_x + (c + 1) * tall, lanes] = mixed_low[
                    at : at + tall
                ]

    for c in range(chunks - 1):
        o_wait(c, 0)
        unmix(c, 0, 5)
    for number, (low, high) in enumerate(halves):
        o_wait(chunks - 1, number)
        unmix(chunks - 1, low, high)
        for m in range(low, high):
            out = along_x(mix[m], mix[m, :width_x], x_ref, low_ref)
            for z in range(depth):
                result_ref[0, m, z] = out[:, z * width_y : (z + 1) * width_y]

    others = spaces - 1
    if chunks > 2:
        bulk(in_send.at[2:chunks, 0:others, 1:5], in_ss[last_left])
    pl.when(helper)(lambda: bulk(in_send.at[0, 0:others, 5:6], first_in_ss))
    pl.when(helping)(lambda: bulk(first_hat, first_ss))
    bulk(o_send.at[:, 0:others], o_ss)
    bulk(steps.at[0 : group - 1], step_ss)

    @pl.when(place < slices - 1)
    def _():
        bulk(ghat, h_ss)
        bulk(z_send.at[:, 0 : group - 1], z_ss)

    pl.when(family < last_group)(lambda: bulk(s_send, s_ss))
    fewer = jnp.logical_and(family == 0, place > 0)
    if group > 2:
        pl.when(fewer)(lambda: bulk(r_send.at[:, 0 : group - 2], r_ss))
    pl.when(jnp.logical_not(fewer))(lambda: bulk(r_send.at[:, 0 : group - 1], r_ss))


def body(initial, start_guess, forcing, step_size):
    depth, width_x, width_y = initial.shape
    spaces, slices = lax.axis_size("space"), lax.axis_size("tm")
    length_z = depth * spaces
    chunks = CHUNKS
    rows = width_x // spaces // chunks
    group = max(1, min(GROUP, slices // 2))
    block = length_z * rows // group
    dims = (spaces, slices, chunks, depth, length_z, rows, width_y, group, block)

    def pair(length):
        return split_pair(jnp.asarray(sine(length), jnp.float32))

    x_high, x_low = pair(width_x)
    y_high, y_low = pair(width_y)
    x_twice = jnp.concatenate([x_high, x_high], axis=1)
    w = jnp.concatenate(
        [
            jnp.concatenate([y_high, y_low], axis=1),
            jnp.concatenate([y_high, jnp.zeros_like(y_low)], axis=1),
        ],
        axis=0,
    )
    sides = jnp.asarray(eigen(width_x)[:, None] + eigen(width_y)[None, :], jnp.float32)
    f32, b16 = jnp.float32, jnp.bfloat16
    flat = length_z * rows
    dma = pltpu.SemaphoreType.DMA
    vmem = pl.BlockSpec(memory_space=pltpu.VMEM)
    hbm = pl.BlockSpec(memory_space=pl.ANY)
    return pl.pallas_call(
        functools.partial(kernel, dims),
        out_shape=pltpu.VMEM((1, 5, depth, width_x, width_y), f32),
        in_specs=[pl.BlockSpec(memory_space=pltpu.SMEM)] + [hbm] * 7,
        out_specs=vmem,
        scratch_shapes=[
            pltpu.VMEM((depth, width_x, width_y), f32),
            pltpu.VMEM((depth, width_x, width_y), f32),
            pltpu.VMEM((5, depth, width_x, width_y), f32),
            pltpu.VMEM((width_x, 2 * width_x), b16),
            pltpu.VMEM((width_x, width_x), b16),
            pltpu.VMEM((2 * width_y, 2 * width_y), b16),
            pltpu.VMEM((width_x, width_y), f32),
            pltpu.VMEM((chunks, spaces, 6, depth, rows, width_y), f32),
            pltpu.VMEM((chunks, spaces, 6, depth, rows, width_y), f32),
            pltpu.VMEM((chunks, flat, width_y), f32),
            pltpu.VMEM((chunks, flat, width_y), f32),
            pltpu.VMEM((chunks, flat, width_y), f32),
            pltpu.VMEM((8, width_y), f32),
            pltpu.VMEM((group, 8, width_y), f32),
            pltpu.VMEM((flat, width_y), f32),
            pltpu.VMEM((chunks, 4, flat, width_y), f32),
            pltpu.VMEM((chunks, 4, flat, width_y), f32),
            pltpu.VMEM((chunks, 4, flat, width_y), f32),
            pltpu.VMEM((chunks, group, 2, block, width_y), f32),
            pltpu.VMEM((chunks, group, 2, block, width_y), f32),
            pltpu.VMEM((chunks, group, block, width_y), f32),
            pltpu.VMEM((chunks, group, block, width_y), f32),
            pltpu.VMEM((chunks, group, 2, block, width_y), f32),
            pltpu.VMEM((chunks, group, 2, block, width_y), f32),
            pltpu.VMEM((chunks, 2, block, width_y), f32),
            pltpu.VMEM((chunks, 2, block, width_y), f32),
            pltpu.VMEM((chunks, spaces, 5, depth, rows, width_y), f32),
            pltpu.VMEM((chunks, spaces, 5, depth, rows, width_y), f32),
            pltpu.VMEM((5, 2 * width_x, depth * width_y), b16),
            dma((7,)),
            dma((chunks, 2)),
            dma((chunks,)),
            dma((chunks, 2)),
            dma((chunks,)),
            dma((chunks,)),
            dma((chunks + 1,)),
            dma((14,)),
            pltpu.SemaphoreType.REGULAR((3,)),
        ],
        compiler_params=pltpu.CompilerParams(collective_id=0, has_side_effects=True),
    )(step_size, initial, start_guess, forcing, x_twice, x_low, w, sides)


def solution(mesh):
    in_specs = (
        P("space", None, None),
        P("tm", "space", None, None),
        P("tm", None, "space", None, None),
        P("tm"),
    )
    out_specs = P("tm", None, "space", None, None)
    return jax.shard_map(body, mesh=mesh, in_specs=in_specs, out_specs=out_specs, check_vma=False)
```

```python
import functools
import math

import jax
import jax.numpy as jnp
import numpy as np
from jax import lax
from jax.experimental import pallas as pl
from jax.experimental.pallas import tpu as pltpu
from jax.sharding import PartitionSpec as P

MESH = pl.DeviceIdType.MESH
CHUNKS = 4
GROUP = 8

def node_tables():
    radical = math.sqrt(3.0 / 7.0)
    node_times = [0.0, (1.0 - radical) / 2.0, 0.5, (1.0 + radical) / 2.0, 1.0]
    integrals = np.zeros((4, 5))
    for column in range(5):
        coeffs = [1.0]
        for other_index in range(5):
            if other_index == column:
                continue
            other_time = node_times[other_index]
            scaling = node_times[column] - other_time
            grown = [0.0] * (len(coeffs) + 1)
            for exponent in range(len(coeffs)):
                grown[exponent + 1] += coeffs[exponent] / scaling
                grown[exponent] -= coeffs[exponent] * other_time / scaling
            coeffs = grown
        for section in range(4):
            integrals[section, column] = sum(
                (
                    coeffs[exponent]
                    * (
                        node_times[section + 1] ** (exponent + 1)
                        - node_times[section] ** (exponent + 1)
                    )
                    / (exponent + 1)
                    for exponent in range(len(coeffs))
                )
            )
    coarse = [0.0, 0.5, 1.0]
    interp = np.zeros((5, 3))
    for column in range(3):
        for section in range(5):
            weight = 1.0
            for other_index in range(3):
                if other_index != column:
                    weight = (
                        weight
                        * (node_times[section] - coarse[other_index])
                        / (coarse[column] - coarse[other_index])
                    )
            interp[section, column] = weight
    return (np.array(node_times), integrals, interp)


def sine(length):
    k = np.arange(1, length + 1)
    phase = np.outer(k, k) % (2 * (length + 1))
    return math.sqrt(2.0 / (length + 1)) * np.sin(math.pi / (length + 1) * phase)


def eigen(length):
    return 2.0 - 2.0 * np.cos(math.pi / (length + 1) * np.arange(1, length + 1))


def split_pair(value):
    high = value.astype(jnp.bfloat16)
    return high, (value - high.astype(jnp.float32)).astype(jnp.bfloat16)


def dot(a, b):
    return jnp.dot(a, b, preferred_element_type=jnp.float32)


def along_y(field, w_ref):
    width = field.shape[1]
    both = dot(jnp.concatenate(split_pair(field), axis=1), w_ref[...])
    return both[:, :width] + both[:, width:]


def along_x(pair, high, x_ref, low_ref):
    return dot(x_ref[...], pair) + dot(low_ref[...], high)


def lateral(field, x_ref, low_ref, w_ref):
    depth, width_x, width_y = field.shape
    mixed = along_y(field.reshape(depth * width_x, width_y), w_ref)
    mixed = jnp.concatenate([mixed[z * width_x : (z + 1) * width_x] for z in range(depth)], axis=1)
    high, low = split_pair(mixed)
    out = along_x(jnp.concatenate([high, low], axis=0), high, x_ref, low_ref)
    return [out[:, z * width_y : (z + 1) * width_y] for z in range(depth)]


def z_sine(planes):
    count = len(planes)
    table = sine(count)
    half = (count + 1) // 2
    pairs = [
        (planes[z] + planes[count - 1 - z], planes[z] - planes[count - 1 - z])
        if z != count - 1 - z
        else (planes[z], None)
        for z in range(half)
    ]
    out = []
    for k in range(count):
        terms = [
            float(table[k, z]) * pairs[z][k % 2] for z in range(half) if pairs[z][k % 2] is not None
        ]
        total = terms[0]
        for term in terms[1:]:
            total = total + term
        out.append(total)
    return out


def weighted(weights, items):
    total = None
    for weight, item in zip(weights, items):
        weight = float(weight)
        if weight == 0.0 or item is None:
            continue
        term = item if weight == 1.0 else weight * item
        total = term if total is None else total + term
    return total


def sweep(rate, nodes, sources):
    times, integrals, _ = TABLES
    swept = [nodes[0]]
    for m in range(4):
        spacing = float(times[m + 1] - times[m])
        inner = weighted(integrals[m], nodes)
        if m > 0:
            inner = inner + spacing * (swept[m] - nodes[m])
        step = rate * inner
        if swept[m] is not None:
            step = step + swept[m]
        if sources is not None:
            step = step + sources[m]
        swept.append(step)
    first = list(integrals[0] + integrals[1])
    second = list(integrals[2] + integrals[3])
    first[0] -= 0.5
    second[2] -= 0.5
    left = rate * weighted(first, swept)
    right = rate * weighted(second, swept)
    if sources is not None:
        left = left + (sources[0] + sources[1])
        right = right + (sources[2] + sources[3])
    return swept, left, right


def corrected(swept, left, right, middle):
    interp = TABLES[2]
    ending = middle * left + right
    deltas = [None if swept[0] is None else -swept[0], left - swept[2], ending - swept[4]]
    return [
        None,
        swept[1] + weighted(interp[1], deltas),
        left,
        swept[3] + weighted(interp[3], deltas),
        ending,
    ]


def start_gains(middle):
    interp = TABLES[2]
    square = middle * middle
    return [
        None,
        float(interp[1, 0]) + float(interp[1, 1]) * middle + float(interp[1, 2]) * square,
        middle,
        float(interp[3, 0]) + float(interp[3, 1]) * middle + float(interp[3, 2]) * square,
        square,
    ]


def gains_of(rate):
    middle = 1.0 + 0.5 * rate
    gains = start_gains(middle)
    nodes = [jnp.ones_like(middle)] + gains[1:]
    swept, left, right = sweep(rate, nodes, None)
    return gains, corrected(swept, left, right, middle)


TABLES = node_tables()


def kernel(
    dims,
    step_ref, initial_hbm, guess_hbm, forcing_hbm, x_hbm, low_hbm, w_hbm, lateral_hbm,
    result_ref,
    initial, guess, forcing, x_ref, low_ref, w_ref, lateral_ref,
    in_send, in_recv, ghat, hhat, ell, own_step, steps,
    first_hat, gain_c, gain_d, part_b, z_send, z_recv, own_gain, own_cross, r_send, r_recv,
    s_send, s_recv, o_send, o_recv, mix,
    load_sem, in_rs, h_rs, z_rs, s_rs, r_rs, o_rs, sent, signals,
):
    spaces, workers, slices, chunks, depth, length_z, rows, width_y, group, block = dims
    me = lax.axis_index("space")
    place = lax.axis_index("tm")
    _, integrals, _ = TABLES
    width_x = workers * chunks * rows
    seat = me // 2
    sub = 16 if block % 16 == 0 else 8
    everyone = spaces - 2
    last_group = slices // group - 1
    family, mine = place // group, lax.rem(place, group)
    eldest = place - mine
    near_sem, next_sem, open_sem = (signals.at[i] for i in range(3))
    h_ss, step_ss, z_ss, s_ss, r_ss, o_ss, step_rs = (sent.at[i] for i in range(7))
    in_ss = [sent.at[7 + i] for i in range(4)]
    first_in_ss, first_in_rs, first_ss = (sent.at[11 + i] for i in range(3))
    helper = jnp.logical_and(family == 0, mine < chunks)

    barrier = pltpu.get_barrier_semaphore()
    odd = lax.rem(me, 2) == 1
    for i in range(1, spaces):
        peer = lax.rem(me + i, spaces)

        @pl.when(lax.rem(peer, 2) == 1)
        def _():
            pl.semaphore_signal(barrier, inc=1, device_id={"space": peer}, device_id_type=MESH)

    sources = (
        guess_hbm.at[0], w_hbm, x_hbm, low_hbm, forcing_hbm.at[0], initial_hbm, lateral_hbm
    )
    loads = [
        pltpu.make_async_copy(source, target, load_sem.at[i])
        for i, (source, target) in enumerate(
            zip(sources, (guess, w_ref, x_ref, low_ref, forcing, initial, lateral_ref))
        )
    ]
    for load in loads:
        load.start()
    load_guess, load_w, load_x, load_low, load_forcing, load_initial, load_lateral = loads

    step = step_ref[0]
    own_step[...] = jnp.full(own_step.shape, step, jnp.float32)
    steps[mine] = jnp.full(own_step.shape, step, jnp.float32)

    def bulk(ref, sem):
        pltpu.make_async_copy(ref, ref, sem).wait()

    def low_of(c, worker):
        return (c * workers + worker) * rows

    def put(field, slot):
        planes = lateral(field, x_ref, low_ref, w_ref)
        for target in range(workers):
            for c in range(chunks):
                low = low_of(c, target)
                for z in range(depth):
                    in_send[c, target, slot, z] = planes[z][low : low + rows]

    def keep(c, low, high):
        in_recv[c, me, low:high] = in_send[c, seat, low:high]

    def in_start(c, low, high, left, landed):
        for worker in range(workers):
            peer = 2 * worker + 1

            @pl.when(me != peer)
            def _():
                pltpu.make_async_remote_copy(
                    src_ref=in_send.at[c, worker, low:high],
                    dst_ref=in_recv.at[c, me, low:high],
                    send_sem=left,
                    recv_sem=landed,
                    device_id={"space": peer},
                    device_id_type=MESH,
                ).start()

    def by_role(action):
        pl.when(odd)(lambda: action(workers - 1))
        pl.when(jnp.logical_not(odd))(lambda: action(workers))

    def in_wait(c, low, high, landed):
        bulk(in_recv.at[c, 0 : spaces - 1, low:high], landed)

    load_guess.wait()
    load_w.wait()
    load_x.wait()
    load_low.wait()
    put(guess[...], 0)

    @pl.when(odd)
    def _():
        pl.semaphore_wait(barrier, spaces - 1)
        pl.semaphore_signal(near_sem, inc=1, device_id={"space": me - 1}, device_id_type=MESH)

    @pl.when(jnp.logical_not(odd))
    def _():
        pl.semaphore_wait(near_sem, 1)

    def guess_start(c):
        in_start(c, 0, 1, in_ss[0], in_rs.at[c, 0])

    for c in range(chunks // 2):
        guess_start(c)

    def greet(target):
        pl.semaphore_signal(barrier, inc=1, device_id={"tm": target}, device_id_type=MESH)

    @pl.when(me == 0)
    def _():
        pl.when(place > 0)(lambda: greet(place - 1))

        @pl.when(place == 0)
        def _():
            for other in range(1, min(chunks, group)):
                greet(other)

    def relatives(action):
        for i in range(1, group):
            action(lax.rem(mine + i, group))

    @pl.when(me == everyone)
    def _():
        relatives(lambda other: greet(eldest + other))
        pl.when(family > 0)(lambda: greet(place - group))

    def tell(sem):
        for worker in range(workers):
            pl.semaphore_signal(
                sem, inc=1, device_id={"space": 2 * worker + 1}, device_id_type=MESH
            )

    load_initial.wait()

    @pl.when(helper)
    def _():
        put(initial[...], 5)
        in_start(mine, 5, 6, first_in_ss, first_in_rs)
        pl.when(odd)(lambda: keep(mine, 5, 6))

    for c in range(chunks // 2, chunks):
        guess_start(c)
    load_forcing.wait()
    for m in range(4):
        put(step * weighted(integrals[m], [forcing[j] for j in range(5)]), m + 1)

    last_left = 3

    def forcing_start(c):
        in_start(c, 1, 5, in_ss[min(c + 1, last_left)], in_rs.at[c, 1])

    def forcing_left(c):
        by_role(lambda n: bulk(in_send.at[c, 0:n, 1:5], in_ss[c + 1]))

    forcing_start(0)

    def guess_left():
        by_role(lambda n: bulk(in_send.at[:, 0:n, 0:1], in_ss[0]))

    helping = jnp.logical_and(helper, place > 0)
    hands = jnp.logical_or(helping, place < slices - 1)

    @pl.when(jnp.logical_not(odd))
    def _():
        @pl.when(me == 0)
        def _():
            both = jnp.logical_and(helping, place < slices - 1)
            pl.when(both)(lambda: pl.semaphore_wait(barrier, 2))
            pl.when(jnp.logical_and(hands, jnp.logical_not(both)))(
                lambda: pl.semaphore_wait(barrier, 1)
            )
            pl.when(hands)(lambda: tell(next_sem))

        guess_left()
        for c in range(1, chunks):
            if 1 < c < last_left + 1:
                forcing_left(c - 2)
            forcing_start(c)

            if c == 2:
                @pl.when(me == everyone)
                def _():
                    pl.when(family < last_group)(lambda: pl.semaphore_wait(barrier, group))
                    pl.when(family == last_group)(lambda: pl.semaphore_wait(barrier, group - 1))
                    tell(open_sem)

    halves = ((0, 3), (3, 5))

    def o_groups(c):
        return halves if c == chunks - 1 else ((0, 5),)

    def o_start(c, number):
        low, high = o_groups(c)[number]
        for i in range(1, spaces):
            peer = lax.rem(me + i, spaces)
            pltpu.make_async_remote_copy(
                src_ref=o_send.at[c, peer, low:high],
                dst_ref=o_recv.at[c, seat, low:high],
                send_sem=o_ss,
                recv_sem=o_rs.at[c + number],
                device_id={"space": peer},
                device_id_type=MESH,
            ).start()

    def o_wait(c, number):
        low, high = o_groups(c)[number]
        by_role(lambda n: bulk(o_recv.at[c, 0:n, low:high], o_rs.at[c + number]))

    load_lateral.wait()

    @pl.when(odd)
    def _():
        for c in range(chunks):
            keep(c, 0, 5)

        z_eigen = eigen(length_z)
        for c in range(chunks):
            low = pl.multiple_of(low_of(c, seat), 8)
            base = lateral_ref[pl.ds(low, rows), :]
            for k in range(length_z):
                ell[c, k * rows : (k + 1) * rows] = -(base + float(z_eigen[k]))

        def table(i, carry):
            for c in range(chunks):
                at = pl.ds(pl.multiple_of(i * rows, 8), rows)
                gains, crossed = gains_of(step * ell[c, at])
                for m in range(1, 5):
                    gain_c[c, m - 1, at] = gains[m]
                    gain_d[c, m - 1, at] = crossed[m]
            return carry

        lax.fori_loop(0, length_z, table, 0)

        def planes_of(c, slot):
            return [in_recv[c, z // depth, slot, z % depth] for z in range(length_z)]

        guess_left()
        if chunks > 1:
            forcing_start(1)

        pl.when(hands)(lambda: pl.semaphore_wait(next_sem, 1))
        after = lax.rem(place + 1, slices)

        def hand(source, target, c, left):
            pltpu.make_async_remote_copy(
                src_ref=source,
                dst_ref=hhat.at[c],
                send_sem=left,
                recv_sem=h_rs.at[c],
                device_id={"tm": target},
                device_id_type=MESH,
            ).start()

        def hand_guess(c):
            in_wait(c, 0, 1, in_rs.at[c, 0])
            for k, plane in enumerate(z_sine(planes_of(c, 0))):
                ghat[c, k * rows : (k + 1) * rows] = plane
            pl.when(place < slices - 1)(lambda: hand(ghat.at[c], after, c, h_ss))

        for c in range(chunks // 2):
            hand_guess(c)

        @pl.when(helper)
        def _():
            in_wait(mine, 5, 6, first_in_rs)
            for k, plane in enumerate(z_sine(planes_of(mine, 5))):
                first_hat[k * rows : (k + 1) * rows] = plane

            @pl.when(place == 0)
            def _():
                hhat[0] = first_hat[...]

            pl.when(place > 0)(lambda: hand(first_hat, 0, mine, first_ss))

        def forcing_next(c):
            if c < chunks:
                if c < last_left + 1:
                    forcing_left(c - 2)
                forcing_start(c)

        forcing_next(2)
        for c in range(chunks // 2, chunks):
            hand_guess(c)
        for c in range(3, chunks):
            forcing_next(c)

        pl.semaphore_wait(open_sem, 1)
        relatives(
            lambda other: pltpu.make_async_remote_copy(
                src_ref=own_step,
                dst_ref=steps.at[mine],
                send_sem=step_ss,
                recv_sem=step_rs,
                device_id={"tm": eldest + other},
                device_id_type=MESH,
            ).start()
        )

        youngest = jnp.where(mine == group - 1, 1, 0)

        def z_start(c):
            relatives(
                lambda other: pltpu.make_async_remote_copy(
                    src_ref=z_send.at[c, other],
                    dst_ref=z_recv.at[c, mine],
                    send_sem=z_ss,
                    recv_sem=z_rs.at[c, youngest],
                    device_id={"tm": eldest + other},
                    device_id_type=MESH,
                ).start()
            )

        first = jnp.where(place == 0, 1.0, 0.0).astype(jnp.float32)

        def chunk(c):
            in_wait(c, 1, 5, in_rs.at[c, 1])
            if c == 0:
                pl.when(place > 0)(lambda: bulk(hhat.at[c], h_rs.at[c]))
            else:
                bulk(hhat.at[c], h_rs.at[c])
            fhat = [z_sine(planes_of(c, m + 1)) for m in range(4)]
            for m in range(4):
                for k in range(length_z):
                    part_b[c, m, k * rows : (k + 1) * rows] = fhat[m][k]

            def solve(i, carry):
                for part in range(block // sub):
                    at = pl.ds(pl.multiple_of(i * block + part * sub, 8), sub)
                    here = pl.ds(part * sub, sub)
                    rate = step * ell[c, at]
                    middle = 1.0 + 0.5 * rate
                    guess_hat, start = ghat[c, at], hhat[c, at]
                    sources = [part_b[c, m, at] for m in range(4)]
                    one = sweep(rate, [start] + [guess_hat] * 4, sources)
                    nodes = corrected(*one, middle)
                    rest = corrected(*sweep(rate, nodes, sources), middle)
                    for m in range(1, 5):
                        part_b[c, m - 1, at] = rest[m]
                    seen = first * start
                    gain, cross = gain_c[c, 3, at], gain_d[c, 3, at]
                    z_send[c, i, 0, here] = nodes[4] + gain * seen
                    z_send[c, i, 1, here] = rest[4] + (gain + cross) * seen
                return carry

            lax.fori_loop(0, group, solve, 0, unroll=2)
            pl.when(place < slices - 1)(lambda: z_start(c))
            z_recv[c, mine] = z_send[c, mine]

        def own_tables(c):
            def one(p, carry):
                for part in range(block // sub):
                    at = pl.ds(pl.multiple_of(mine * block + part * sub, 8), sub)
                    here = pl.ds(part * sub, sub)
                    gains, crossed = gains_of(steps[p][0:1] * ell[c, at])
                    own_gain[c, p, here] = gains[4]
                    own_cross[c, p, here] = crossed[4]
                return carry

            lax.fori_loop(0, group, one, 0)

        def r_start(c, other):
            pltpu.make_async_remote_copy(
                src_ref=r_send.at[c, other],
                dst_ref=r_recv.at[c, mine],
                send_sem=r_ss,
                recv_sem=r_rs.at[c],
                device_id={"tm": eldest + other},
                device_id_type=MESH,
            ).start()

        def scan(c):
            if c == 0:
                bulk(steps.at[0 : group - 1], step_rs)
            own_tables(c)

            @pl.when(mine < group - 1)
            def _():
                if group > 2:
                    bulk(z_recv.at[c, 0 : group - 2], z_rs.at[c, 0])

            pl.when(mine == group - 1)(lambda: bulk(z_recv.at[c, 0 : group - 1], z_rs.at[c, 0]))
            pl.when(family > 0)(lambda: bulk(s_recv.at[c], s_rs.at[c]))

            def advance(p, lower, upper):
                gain = own_gain[c, p]
                return (
                    gain * lower + z_recv[c, p, 0],
                    gain * upper + own_cross[c, p] * lower + z_recv[c, p, 1],
                )

            lower, upper = (jnp.where(family > 0, s_recv[c, i], 0.0) for i in range(2))
            for p in range(group):
                r_send[c, p, 0] = lower
                r_send[c, p, 1] = upper
                if p < group - 1:
                    lower, upper = advance(p, lower, upper)

            @pl.when(family < last_group)
            def _():
                pl.when(mine < group - 1)(lambda: bulk(z_recv.at[c, 0], z_rs.at[c, 1]))
                final = advance(group - 1, r_send[c, group - 1, 0], r_send[c, group - 1, 1])
                s_send[c, 0], s_send[c, 1] = final
                pltpu.make_async_remote_copy(
                    src_ref=s_send.at[c],
                    dst_ref=s_recv.at[c],
                    send_sem=s_ss,
                    recv_sem=s_rs.at[c],
                    device_id={"tm": place + group},
                    device_id_type=MESH,
                ).start()

            relatives(lambda other: pl.when(eldest + other > 0)(lambda: r_start(c, other)))
            r_recv[c, mine] = r_send[c, mine]

        def give(c, lower, upper):
            for m in range(5):
                if m == 0:
                    value = upper
                else:
                    value = (
                        gain_c[c, m - 1] * upper + gain_d[c, m - 1] * lower + part_b[c, m - 1]
                    )
                planes = z_sine([value[k * rows : (k + 1) * rows] for k in range(length_z)])
                for z in range(length_z):
                    o_send[c, z // depth, m, z % depth] = planes[z]
                for number, (_, high) in enumerate(o_groups(c)):
                    if high == m + 1:
                        o_start(c, number)
                o_recv[c, seat, m] = o_send[c, me, m]

        def give_first(c):
            own = hhat[c]
            give(c, own, own)

        def give_later(c):
            bulk(r_recv.at[c, 0 : group - 1], r_rs.at[c])
            give(c, *(r_recv[c, :, i].reshape(length_z * rows, width_y) for i in range(2)))

        early = max(0, chunks - 3)
        for c in range(chunks):
            chunk(c)
            if c == early:
                pl.when(place == group - 1)(lambda: scan(0))
            if c == max(0, chunks - 2):
                pl.when(place < group - 1)(lambda: scan(0))
        pl.when(family > 0)(lambda: scan(0))

        @pl.when(place == 0)
        def _():
            for c in range(1, chunks):
                scan(c)
                give_first(c - 1)
            give_first(chunks - 1)

        @pl.when(place > 0)
        def _():
            for c in range(1, chunks):
                scan(c)
                if c >= 2:
                    give_later(c - 2)
            for c in range(max(0, chunks - 2), chunks):
                give_later(c)

    def unmix(c, low, high):
        stacked = jnp.concatenate(
            [
                o_recv[c, s, m, z]
                for m in range(low, high)
                for z in range(depth)
                for s in range(workers)
            ],
            axis=0,
        )
        tall = workers * rows
        mixed_high, mixed_low = split_pair(along_y(stacked, w_ref))
        for m in range(low, high):
            for z in range(depth):
                at = ((m - low) * depth + z) * tall
                lanes = slice(z * width_y, (z + 1) * width_y)
                mix[m, c * tall : (c + 1) * tall, lanes] = mixed_high[at : at + tall]
                mix[m, width_x + c * tall : width_x + (c + 1) * tall, lanes] = mixed_low[
                    at : at + tall
                ]

    for c in range(chunks - 1):
        o_wait(c, 0)
        unmix(c, 0, 5)
    for number, (low, high) in enumerate(halves):
        o_wait(chunks - 1, number)
        unmix(chunks - 1, low, high)
        for m in range(low, high):
            out = along_x(mix[m], mix[m, :width_x], x_ref, low_ref)
            for z in range(depth):
                result_ref[0, m, z] = out[:, z * width_y : (z + 1) * width_y]

    if chunks > 2:
        by_role(lambda n: bulk(in_send.at[2:chunks, 0:n, 1:5], in_ss[last_left]))
    pl.when(helper)(lambda: by_role(lambda n: bulk(in_send.at[0, 0:n, 5:6], first_in_ss)))

    @pl.when(odd)
    def _():
        pl.when(helping)(lambda: bulk(first_hat, first_ss))
        bulk(o_send.at[:, 0 : spaces - 1], o_ss)
        bulk(steps.at[0 : group - 1], step_ss)

        @pl.when(place < slices - 1)
        def _():
            bulk(ghat, h_ss)
            bulk(z_send.at[:, 0 : group - 1], z_ss)

        pl.when(family < last_group)(lambda: bulk(s_send, s_ss))
        fewer = jnp.logical_and(family == 0, place > 0)
        if group > 2:
            pl.when(fewer)(lambda: bulk(r_send.at[:, 0 : group - 2], r_ss))
        pl.when(jnp.logical_not(fewer))(lambda: bulk(r_send.at[:, 0 : group - 1], r_ss))


def body(initial, start_guess, forcing, step_size):
    depth, width_x, width_y = initial.shape
    spaces, slices = lax.axis_size("space"), lax.axis_size("tm")
    length_z = depth * spaces
    chunks = CHUNKS
    workers = spaces // 2
    rows = width_x // workers // chunks
    group = max(1, min(GROUP, slices // 2))
    block = length_z * rows // group
    dims = (spaces, workers, slices, chunks, depth, length_z, rows, width_y, group, block)

    def pair(length):
        return split_pair(jnp.asarray(sine(length), jnp.float32))

    x_high, x_low = pair(width_x)
    y_high, y_low = pair(width_y)
    x_twice = jnp.concatenate([x_high, x_high], axis=1)
    w = jnp.concatenate(
        [
            jnp.concatenate([y_high, y_low], axis=1),
            jnp.concatenate([y_high, jnp.zeros_like(y_low)], axis=1),
        ],
        axis=0,
    )
    sides = jnp.asarray(eigen(width_x)[:, None] + eigen(width_y)[None, :], jnp.float32)
    f32, b16 = jnp.float32, jnp.bfloat16
    flat = length_z * rows
    dma = pltpu.SemaphoreType.DMA
    vmem = pl.BlockSpec(memory_space=pltpu.VMEM)
    hbm = pl.BlockSpec(memory_space=pl.ANY)
    return pl.pallas_call(
        functools.partial(kernel, dims),
        out_shape=pltpu.VMEM((1, 5, depth, width_x, width_y), f32),
        in_specs=[pl.BlockSpec(memory_space=pltpu.SMEM)] + [hbm] * 7,
        out_specs=vmem,
        scratch_shapes=[
            pltpu.VMEM((depth, width_x, width_y), f32),
            pltpu.VMEM((depth, width_x, width_y), f32),
            pltpu.VMEM((5, depth, width_x, width_y), f32),
            pltpu.VMEM((width_x, 2 * width_x), b16),
            pltpu.VMEM((width_x, width_x), b16),
            pltpu.VMEM((2 * width_y, 2 * width_y), b16),
            pltpu.VMEM((width_x, width_y), f32),
            pltpu.VMEM((chunks, workers, 6, depth, rows, width_y), f32),
            pltpu.VMEM((chunks, spaces, 6, depth, rows, width_y), f32),
            pltpu.VMEM((chunks, flat, width_y), f32),
            pltpu.VMEM((chunks, flat, width_y), f32),
            pltpu.VMEM((chunks, flat, width_y), f32),
            pltpu.VMEM((8, width_y), f32),
            pltpu.VMEM((group, 8, width_y), f32),
            pltpu.VMEM((flat, width_y), f32),
            pltpu.VMEM((chunks, 4, flat, width_y), f32),
            pltpu.VMEM((chunks, 4, flat, width_y), f32),
            pltpu.VMEM((chunks, 4, flat, width_y), f32),
            pltpu.VMEM((chunks, group, 2, block, width_y), f32),
            pltpu.VMEM((chunks, group, 2, block, width_y), f32),
            pltpu.VMEM((chunks, group, block, width_y), f32),
            pltpu.VMEM((chunks, group, block, width_y), f32),
            pltpu.VMEM((chunks, group, 2, block, width_y), f32),
            pltpu.VMEM((chunks, group, 2, block, width_y), f32),
            pltpu.VMEM((chunks, 2, block, width_y), f32),
            pltpu.VMEM((chunks, 2, block, width_y), f32),
            pltpu.VMEM((chunks, spaces, 5, depth, rows, width_y), f32),
            pltpu.VMEM((chunks, workers, 5, depth, rows, width_y), f32),
            pltpu.VMEM((5, 2 * width_x, depth * width_y), b16),
            dma((7,)),
            dma((chunks, 2)),
            dma((chunks,)),
            dma((chunks, 2)),
            dma((chunks,)),
            dma((chunks,)),
            dma((chunks + 1,)),
            dma((14,)),
            pltpu.SemaphoreType.REGULAR((3,)),
        ],
        compiler_params=pltpu.CompilerParams(collective_id=0, has_side_effects=True),
    )(step_size, initial, start_guess, forcing, x_twice, x_low, w, sides)


def solution(mesh):
    in_specs = (
        P("space", None, None),
        P("tm", "space", None, None),
        P("tm", None, "space", None, None),
        P("tm"),
    )
    out_specs = P("tm", None, "space", None, None)
    return jax.shard_map(body, mesh=mesh, in_specs=in_specs, out_specs=out_specs, check_vma=False)
```

```python
import functools
import math

import jax
import jax.numpy as jnp
import numpy as np
from jax import lax
from jax.experimental import pallas as pl
from jax.experimental.pallas import tpu as pltpu
from jax.sharding import PartitionSpec as P

MESH = pl.DeviceIdType.MESH
CHUNKS = 4
GROUP = 8

def node_tables():
    radical = math.sqrt(3.0 / 7.0)
    node_times = [0.0, (1.0 - radical) / 2.0, 0.5, (1.0 + radical) / 2.0, 1.0]
    integrals = np.zeros((4, 5))
    for column in range(5):
        coeffs = [1.0]
        for other_index in range(5):
            if other_index == column:
                continue
            other_time = node_times[other_index]
            scaling = node_times[column] - other_time
            grown = [0.0] * (len(coeffs) + 1)
            for exponent in range(len(coeffs)):
                grown[exponent + 1] += coeffs[exponent] / scaling
                grown[exponent] -= coeffs[exponent] * other_time / scaling
            coeffs = grown
        for section in range(4):
            integrals[section, column] = sum(
                (
                    coeffs[exponent]
                    * (
                        node_times[section + 1] ** (exponent + 1)
                        - node_times[section] ** (exponent + 1)
                    )
                    / (exponent + 1)
                    for exponent in range(len(coeffs))
                )
            )
    coarse = [0.0, 0.5, 1.0]
    interp = np.zeros((5, 3))
    for column in range(3):
        for section in range(5):
            weight = 1.0
            for other_index in range(3):
                if other_index != column:
                    weight = (
                        weight
                        * (node_times[section] - coarse[other_index])
                        / (coarse[column] - coarse[other_index])
                    )
            interp[section, column] = weight
    return (np.array(node_times), integrals, interp)


def sine(length):
    k = np.arange(1, length + 1)
    phase = np.outer(k, k) % (2 * (length + 1))
    return math.sqrt(2.0 / (length + 1)) * np.sin(math.pi / (length + 1) * phase)


def eigen(length):
    return 2.0 - 2.0 * np.cos(math.pi / (length + 1) * np.arange(1, length + 1))


def split_pair(value):
    high = value.astype(jnp.bfloat16)
    return high, (value - high.astype(jnp.float32)).astype(jnp.bfloat16)


def dot(a, b):
    return jnp.dot(a, b, preferred_element_type=jnp.float32)


def along_y(field, w_ref):
    width = field.shape[1]
    both = dot(jnp.concatenate(split_pair(field), axis=1), w_ref[...])
    return both[:, :width] + both[:, width:]


def along_x(pair, high, x_ref, low_ref):
    return dot(x_ref[...], pair) + dot(low_ref[...], high)


def lateral(field, x_ref, low_ref, w_ref):
    depth, width_x, width_y = field.shape
    mixed = along_y(field.reshape(depth * width_x, width_y), w_ref)
    mixed = jnp.concatenate([mixed[z * width_x : (z + 1) * width_x] for z in range(depth)], axis=1)
    high, low = split_pair(mixed)
    out = along_x(jnp.concatenate([high, low], axis=0), high, x_ref, low_ref)
    return [out[:, z * width_y : (z + 1) * width_y] for z in range(depth)]


def z_sine(planes):
    count = len(planes)
    table = sine(count)
    half = (count + 1) // 2
    pairs = [
        (planes[z] + planes[count - 1 - z], planes[z] - planes[count - 1 - z])
        if z != count - 1 - z
        else (planes[z], None)
        for z in range(half)
    ]
    out = []
    for k in range(count):
        terms = [
            float(table[k, z]) * pairs[z][k % 2] for z in range(half) if pairs[z][k % 2] is not None
        ]
        total = terms[0]
        for term in terms[1:]:
            total = total + term
        out.append(total)
    return out


def weighted(weights, items):
    total = None
    for weight, item in zip(weights, items):
        weight = float(weight)
        if weight == 0.0 or item is None:
            continue
        term = item if weight == 1.0 else weight * item
        total = term if total is None else total + term
    return total


def sweep(rate, nodes, sources):
    times, integrals, _ = TABLES
    swept = [nodes[0]]
    for m in range(4):
        spacing = float(times[m + 1] - times[m])
        inner = weighted(integrals[m], nodes)
        if m > 0:
            inner = inner + spacing * (swept[m] - nodes[m])
        step = rate * inner
        if swept[m] is not None:
            step = step + swept[m]
        if sources is not None:
            step = step + sources[m]
        swept.append(step)
    first = list(integrals[0] + integrals[1])
    second = list(integrals[2] + integrals[3])
    first[0] -= 0.5
    second[2] -= 0.5
    left = rate * weighted(first, swept)
    right = rate * weighted(second, swept)
    if sources is not None:
        left = left + (sources[0] + sources[1])
        right = right + (sources[2] + sources[3])
    return swept, left, right


def corrected(swept, left, right, middle):
    interp = TABLES[2]
    ending = middle * left + right
    deltas = [None if swept[0] is None else -swept[0], left - swept[2], ending - swept[4]]
    return [
        None,
        swept[1] + weighted(interp[1], deltas),
        left,
        swept[3] + weighted(interp[3], deltas),
        ending,
    ]


def start_gains(middle):
    interp = TABLES[2]
    square = middle * middle
    return [
        None,
        float(interp[1, 0]) + float(interp[1, 1]) * middle + float(interp[1, 2]) * square,
        middle,
        float(interp[3, 0]) + float(interp[3, 1]) * middle + float(interp[3, 2]) * square,
        square,
    ]


def gains_of(rate):
    middle = 1.0 + 0.5 * rate
    gains = start_gains(middle)
    nodes = [jnp.ones_like(middle)] + gains[1:]
    swept, left, right = sweep(rate, nodes, None)
    return gains, corrected(swept, left, right, middle)


TABLES = node_tables()


def kernel(
    dims,
    step_ref, initial_hbm, guess_hbm, forcing_hbm, x_hbm, low_hbm, w_hbm, lateral_hbm,
    result_ref,
    initial, guess, forcing, x_ref, low_ref, w_ref, lateral_ref,
    in_send, in_recv, ghat, hhat, ell, own_step, steps,
    first_hat, gain_c, gain_d, part_b, z_send, z_recv, own_gain, own_cross, r_send, r_recv,
    s_send, s_recv, o_send, o_recv, mix,
    load_sem, in_rs, h_rs, z_rs, s_rs, r_rs, o_rs, sent, signals,
):
    spaces, workers, slices, chunks, depth, length_z, rows, width_y, group, block = dims
    me = lax.axis_index("space")
    place = lax.axis_index("tm")
    _, integrals, _ = TABLES
    width_x = workers * chunks * rows
    seat = me // 2
    sub = 16 if block % 16 == 0 else 8
    everyone = spaces - 2
    last_group = slices // group - 1
    family, mine = place // group, lax.rem(place, group)
    eldest = place - mine
    near_sem, next_sem, open_sem = (signals.at[i] for i in range(3))
    h_ss, step_ss, z_ss, s_ss, r_ss, o_ss, step_rs = (sent.at[i] for i in range(7))
    in_ss = [sent.at[7 + i] for i in range(4)]
    first_in_ss, first_in_rs, first_ss = (sent.at[11 + i] for i in range(3))
    helper = jnp.logical_and(family == 0, mine < chunks)

    barrier = pltpu.get_barrier_semaphore()
    odd = lax.rem(me, 2) == 1
    for i in range(1, spaces):
        peer = lax.rem(me + i, spaces)

        @pl.when(lax.rem(peer, 2) == 1)
        def _():
            pl.semaphore_signal(barrier, inc=1, device_id={"space": peer}, device_id_type=MESH)

    sources = (
        guess_hbm.at[0], w_hbm, x_hbm, low_hbm, forcing_hbm.at[0], initial_hbm, lateral_hbm
    )
    loads = [
        pltpu.make_async_copy(source, target, load_sem.at[i])
        for i, (source, target) in enumerate(
            zip(sources, (guess, w_ref, x_ref, low_ref, forcing, initial, lateral_ref))
        )
    ]
    for load in loads:
        load.start()
    load_guess, load_w, load_x, load_low, load_forcing, load_initial, load_lateral = loads

    step = step_ref[0]
    own_step[...] = jnp.full(own_step.shape, step, jnp.float32)
    steps[mine] = jnp.full(own_step.shape, step, jnp.float32)

    def bulk(ref, sem):
        pltpu.make_async_copy(ref, ref, sem).wait()

    def low_of(c, worker):
        return (c * workers + worker) * rows

    def put(field, slot):
        planes = lateral(field, x_ref, low_ref, w_ref)
        for target in range(workers):
            for c in range(chunks):
                low = low_of(c, target)
                for z in range(depth):
                    in_send[c, target, slot, z] = planes[z][low : low + rows]

    def keep(c, low, high):
        in_recv[c, me, low:high] = in_send[c, seat, low:high]

    def in_start(c, low, high, left, landed):
        for worker in range(workers):
            peer = 2 * worker + 1

            @pl.when(me != peer)
            def _():
                pltpu.make_async_remote_copy(
                    src_ref=in_send.at[c, worker, low:high],
                    dst_ref=in_recv.at[c, me, low:high],
                    send_sem=left,
                    recv_sem=landed,
                    device_id={"space": peer},
                    device_id_type=MESH,
                ).start()

    def by_role(action):
        pl.when(odd)(lambda: action(workers - 1))
        pl.when(jnp.logical_not(odd))(lambda: action(workers))

    def in_wait(c, low, high, landed):
        bulk(in_recv.at[c, 0 : spaces - 1, low:high], landed)

    load_guess.wait()
    load_w.wait()
    load_x.wait()
    load_low.wait()
    put(guess[...], 0)

    @pl.when(odd)
    def _():
        pl.semaphore_wait(barrier, spaces - 1)
        pl.semaphore_signal(near_sem, inc=1, device_id={"space": me - 1}, device_id_type=MESH)

    @pl.when(jnp.logical_not(odd))
    def _():
        pl.semaphore_wait(near_sem, 1)

    def guess_start(c):
        in_start(c, 0, 1, in_ss[0], in_rs.at[c, 0])

    for c in range(chunks // 2):
        guess_start(c)

    def greet(target):
        pl.semaphore_signal(barrier, inc=1, device_id={"tm": target}, device_id_type=MESH)

    @pl.when(me == 0)
    def _():
        pl.when(place > 0)(lambda: greet(place - 1))

        @pl.when(place == 0)
        def _():
            for other in range(1, min(chunks, group)):
                greet(other)

    def relatives(action):
        for i in range(1, group):
            action(lax.rem(mine + i, group))

    @pl.when(me == everyone)
    def _():
        relatives(lambda other: greet(eldest + other))
        pl.when(family > 0)(lambda: greet(place - group))

    def tell(sem):
        for worker in range(workers):
            pl.semaphore_signal(
                sem, inc=1, device_id={"space": 2 * worker + 1}, device_id_type=MESH
            )

    load_initial.wait()

    @pl.when(helper)
    def _():
        put(initial[...], 5)
        in_start(mine, 5, 6, first_in_ss, first_in_rs)
        pl.when(odd)(lambda: keep(mine, 5, 6))

    for c in range(chunks // 2, chunks):
        guess_start(c)
    load_forcing.wait()
    for m in range(4):
        put(step * weighted(integrals[m], [forcing[j] for j in range(5)]), m + 1)

    last_left = 3

    def forcing_start(c):
        in_start(c, 1, 5, in_ss[min(c + 1, last_left)], in_rs.at[c, 1])

    def forcing_left(c):
        by_role(lambda n: bulk(in_send.at[c, 0:n, 1:5], in_ss[c + 1]))

    forcing_start(0)

    def guess_left():
        by_role(lambda n: bulk(in_send.at[:, 0:n, 0:1], in_ss[0]))

    helping = jnp.logical_and(helper, place > 0)
    hands = jnp.logical_or(helping, place < slices - 1)

    @pl.when(jnp.logical_not(odd))
    def _():
        @pl.when(me == 0)
        def _():
            both = jnp.logical_and(helping, place < slices - 1)
            pl.when(both)(lambda: pl.semaphore_wait(barrier, 2))
            pl.when(jnp.logical_and(hands, jnp.logical_not(both)))(
                lambda: pl.semaphore_wait(barrier, 1)
            )
            pl.when(hands)(lambda: tell(next_sem))

        guess_left()
        for c in range(1, chunks):
            if 1 < c < last_left + 1:
                forcing_left(c - 2)
            forcing_start(c)

            if c == 2:
                @pl.when(me == everyone)
                def _():
                    pl.when(family < last_group)(lambda: pl.semaphore_wait(barrier, group))
                    pl.when(family == last_group)(lambda: pl.semaphore_wait(barrier, group - 1))
                    tell(open_sem)

    halves = ((0, 3), (3, 5))

    def o_groups(c):
        return halves if c == chunks - 1 else ((0, 5),)

    def o_start(c, number):
        low, high = o_groups(c)[number]
        for i in range(1, spaces):
            peer = lax.rem(me + i, spaces)
            pltpu.make_async_remote_copy(
                src_ref=o_send.at[c, peer, low:high],
                dst_ref=o_recv.at[c, seat, low:high],
                send_sem=o_ss,
                recv_sem=o_rs.at[c + number],
                device_id={"space": peer},
                device_id_type=MESH,
            ).start()

    def o_wait(c, number):
        low, high = o_groups(c)[number]
        by_role(lambda n: bulk(o_recv.at[c, 0:n, low:high], o_rs.at[c + number]))

    load_lateral.wait()

    @pl.when(odd)
    def _():
        for c in range(chunks):
            keep(c, 0, 5)

        z_eigen = eigen(length_z)
        for c in range(chunks):
            low = pl.multiple_of(low_of(c, seat), 8)
            base = lateral_ref[pl.ds(low, rows), :]
            for k in range(length_z):
                ell[c, k * rows : (k + 1) * rows] = -(base + float(z_eigen[k]))

        def table(i, carry):
            for c in range(chunks):
                at = pl.ds(pl.multiple_of(i * rows, 8), rows)
                gains, crossed = gains_of(step * ell[c, at])
                for m in range(1, 5):
                    gain_c[c, m - 1, at] = gains[m]
                    gain_d[c, m - 1, at] = crossed[m]
            return carry

        lax.fori_loop(0, length_z, table, 0)

        def planes_of(c, slot):
            return [in_recv[c, z // depth, slot, z % depth] for z in range(length_z)]

        guess_left()
        if chunks > 1:
            forcing_start(1)

        pl.when(hands)(lambda: pl.semaphore_wait(next_sem, 1))
        after = lax.rem(place + 1, slices)

        def hand(source, target, c, left):
            pltpu.make_async_remote_copy(
                src_ref=source,
                dst_ref=hhat.at[c],
                send_sem=left,
                recv_sem=h_rs.at[c],
                device_id={"tm": target},
                device_id_type=MESH,
            ).start()

        def hand_guess(c):
            in_wait(c, 0, 1, in_rs.at[c, 0])
            for k, plane in enumerate(z_sine(planes_of(c, 0))):
                ghat[c, k * rows : (k + 1) * rows] = plane
            pl.when(place < slices - 1)(lambda: hand(ghat.at[c], after, c, h_ss))

        for c in range(chunks // 2):
            hand_guess(c)

        @pl.when(helper)
        def _():
            in_wait(mine, 5, 6, first_in_rs)
            for k, plane in enumerate(z_sine(planes_of(mine, 5))):
                first_hat[k * rows : (k + 1) * rows] = plane

            @pl.when(place == 0)
            def _():
                hhat[0] = first_hat[...]

            pl.when(place > 0)(lambda: hand(first_hat, 0, mine, first_ss))

        def forcing_next(c):
            if c < chunks:
                if c < last_left + 1:
                    forcing_left(c - 2)
                forcing_start(c)

        forcing_next(2)
        for c in range(chunks // 2, chunks):
            hand_guess(c)
        for c in range(3, chunks):
            forcing_next(c)

        pl.semaphore_wait(open_sem, 1)
        relatives(
            lambda other: pltpu.make_async_remote_copy(
                src_ref=own_step,
                dst_ref=steps.at[mine],
                send_sem=step_ss,
                recv_sem=step_rs,
                device_id={"tm": eldest + other},
                device_id_type=MESH,
            ).start()
        )

        youngest = jnp.where(mine == group - 1, 1, 0)

        def z_start(c, other):
            pltpu.make_async_remote_copy(
                src_ref=z_send.at[c, other],
                dst_ref=z_recv.at[c, mine],
                send_sem=z_ss,
                recv_sem=z_rs.at[c, youngest],
                device_id={"tm": eldest + other},
                device_id_type=MESH,
            ).start()

        first = jnp.where(place == 0, 1.0, 0.0).astype(jnp.float32)

        def chunk(c):
            in_wait(c, 1, 5, in_rs.at[c, 1])
            if c == 0:
                pl.when(place > 0)(lambda: bulk(hhat.at[c], h_rs.at[c]))
            else:
                bulk(hhat.at[c], h_rs.at[c])
            fhat = [z_sine(planes_of(c, m + 1)) for m in range(4)]
            for m in range(4):
                for k in range(length_z):
                    part_b[c, m, k * rows : (k + 1) * rows] = fhat[m][k]

            def solve(i, carry):
                for part in range(block // sub):
                    at = pl.ds(pl.multiple_of(i * block + part * sub, 8), sub)
                    here = pl.ds(part * sub, sub)
                    rate = step * ell[c, at]
                    middle = 1.0 + 0.5 * rate
                    guess_hat, start = ghat[c, at], hhat[c, at]
                    sources = [part_b[c, m, at] for m in range(4)]
                    one = sweep(rate, [start] + [guess_hat] * 4, sources)
                    nodes = corrected(*one, middle)
                    rest = corrected(*sweep(rate, nodes, sources), middle)
                    for m in range(1, 5):
                        part_b[c, m - 1, at] = rest[m]
                    seen = first * start
                    gain, cross = gain_c[c, 3, at], gain_d[c, 3, at]
                    z_send[c, i, 0, here] = nodes[4] + gain * seen
                    z_send[c, i, 1, here] = rest[4] + (gain + cross) * seen
                return carry

            half = group // 2
            for i in [half] + [k for k in range(1, group) if k != half]:
                other = lax.rem(mine + i, group)
                solve(other, 0)
                pl.when(place < slices - 1)(lambda: z_start(c, other))
            solve(mine, 0)
            z_recv[c, mine] = z_send[c, mine]

        def own_tables(c):
            def one(p, carry):
                for part in range(block // sub):
                    at = pl.ds(pl.multiple_of(mine * block + part * sub, 8), sub)
                    here = pl.ds(part * sub, sub)
                    gains, crossed = gains_of(steps[p][0:1] * ell[c, at])
                    own_gain[c, p, here] = gains[4]
                    own_cross[c, p, here] = crossed[4]
                return carry

            lax.fori_loop(0, group, one, 0)

        def r_start(c, other):
            pltpu.make_async_remote_copy(
                src_ref=r_send.at[c, other],
                dst_ref=r_recv.at[c, mine],
                send_sem=r_ss,
                recv_sem=r_rs.at[c],
                device_id={"tm": eldest + other},
                device_id_type=MESH,
            ).start()

        def scan(c):
            if c == 0:
                bulk(steps.at[0 : group - 1], step_rs)
            own_tables(c)

            @pl.when(mine < group - 1)
            def _():
                if group > 2:
                    bulk(z_recv.at[c, 0 : group - 2], z_rs.at[c, 0])

            pl.when(mine == group - 1)(lambda: bulk(z_recv.at[c, 0 : group - 1], z_rs.at[c, 0]))
            pl.when(family > 0)(lambda: bulk(s_recv.at[c], s_rs.at[c]))

            def advance(p, lower, upper):
                gain = own_gain[c, p]
                return (
                    gain * lower + z_recv[c, p, 0],
                    gain * upper + own_cross[c, p] * lower + z_recv[c, p, 1],
                )

            lower, upper = (jnp.where(family > 0, s_recv[c, i], 0.0) for i in range(2))
            for p in range(group):
                r_send[c, p, 0] = lower
                r_send[c, p, 1] = upper
                if p < group - 1:
                    lower, upper = advance(p, lower, upper)

            @pl.when(family < last_group)
            def _():
                pl.when(mine < group - 1)(lambda: bulk(z_recv.at[c, 0], z_rs.at[c, 1]))
                final = advance(group - 1, r_send[c, group - 1, 0], r_send[c, group - 1, 1])
                s_send[c, 0], s_send[c, 1] = final
                pltpu.make_async_remote_copy(
                    src_ref=s_send.at[c],
                    dst_ref=s_recv.at[c],
                    send_sem=s_ss,
                    recv_sem=s_rs.at[c],
                    device_id={"tm": place + group},
                    device_id_type=MESH,
                ).start()

            relatives(lambda other: pl.when(eldest + other > 0)(lambda: r_start(c, other)))
            r_recv[c, mine] = r_send[c, mine]

        def give(c, lower, upper):
            for m in range(5):
                if m == 0:
                    value = upper
                else:
                    value = (
                        gain_c[c, m - 1] * upper + gain_d[c, m - 1] * lower + part_b[c, m - 1]
                    )
                planes = z_sine([value[k * rows : (k + 1) * rows] for k in range(length_z)])
                for z in range(length_z):
                    o_send[c, z // depth, m, z % depth] = planes[z]
                for number, (_, high) in enumerate(o_groups(c)):
                    if high == m + 1:
                        o_start(c, number)
                o_recv[c, seat, m] = o_send[c, me, m]

        def give_first(c):
            own = hhat[c]
            give(c, own, own)

        def give_later(c):
            bulk(r_recv.at[c, 0 : group - 1], r_rs.at[c])
            give(c, *(r_recv[c, :, i].reshape(length_z * rows, width_y) for i in range(2)))

        early = max(0, chunks - 3)
        for c in range(chunks):
            chunk(c)
            if c == early:
                pl.when(place == group - 1)(lambda: scan(0))
            if c == max(0, chunks - 2):
                pl.when(place < group - 1)(lambda: scan(0))
        pl.when(family > 0)(lambda: scan(0))

        @pl.when(place == 0)
        def _():
            for c in range(1, chunks):
                scan(c)
                give_first(c - 1)
            give_first(chunks - 1)

        def later(lag):
            for c in range(1, chunks):
                scan(c)
                if c >= lag:
                    give_later(c - lag)
            for c in range(max(0, chunks - lag), chunks):
                give_later(c)

        soon = jnp.logical_and(family > 0, mine < group // 2)
        pl.when(soon)(lambda: later(1))
        pl.when(jnp.logical_and(place > 0, jnp.logical_not(soon)))(lambda: later(2))

    def unmix(c, low, high):
        stacked = jnp.concatenate(
            [
                o_recv[c, s, m, z]
                for m in range(low, high)
                for z in range(depth)
                for s in range(workers)
            ],
            axis=0,
        )
        tall = workers * rows
        mixed_high, mixed_low = split_pair(along_y(stacked, w_ref))
        for m in range(low, high):
            for z in range(depth):
                at = ((m - low) * depth + z) * tall
                lanes = slice(z * width_y, (z + 1) * width_y)
                mix[m, c * tall : (c + 1) * tall, lanes] = mixed_high[at : at + tall]
                mix[m, width_x + c * tall : width_x + (c + 1) * tall, lanes] = mixed_low[
                    at : at + tall
                ]

    for c in range(chunks - 1):
        o_wait(c, 0)
        unmix(c, 0, 5)
    for number, (low, high) in enumerate(halves):
        o_wait(chunks - 1, number)
        unmix(chunks - 1, low, high)
        for m in range(low, high):
            out = along_x(mix[m], mix[m, :width_x], x_ref, low_ref)
            for z in range(depth):
                result_ref[0, m, z] = out[:, z * width_y : (z + 1) * width_y]

    if chunks > 2:
        by_role(lambda n: bulk(in_send.at[2:chunks, 0:n, 1:5], in_ss[last_left]))
    pl.when(helper)(lambda: by_role(lambda n: bulk(in_send.at[0, 0:n, 5:6], first_in_ss)))

    @pl.when(odd)
    def _():
        pl.when(helping)(lambda: bulk(first_hat, first_ss))
        bulk(o_send.at[:, 0 : spaces - 1], o_ss)
        bulk(steps.at[0 : group - 1], step_ss)

        @pl.when(place < slices - 1)
        def _():
            bulk(ghat, h_ss)
            bulk(z_send.at[:, 0 : group - 1], z_ss)

        pl.when(family < last_group)(lambda: bulk(s_send, s_ss))
        fewer = jnp.logical_and(family == 0, place > 0)
        if group > 2:
            pl.when(fewer)(lambda: bulk(r_send.at[:, 0 : group - 2], r_ss))
        pl.when(jnp.logical_not(fewer))(lambda: bulk(r_send.at[:, 0 : group - 1], r_ss))


def body(initial, start_guess, forcing, step_size):
    depth, width_x, width_y = initial.shape
    spaces, slices = lax.axis_size("space"), lax.axis_size("tm")
    length_z = depth * spaces
    chunks = CHUNKS
    workers = spaces // 2
    rows = width_x // workers // chunks
    group = max(1, min(GROUP, slices // 2))
    block = length_z * rows // group
    dims = (spaces, workers, slices, chunks, depth, length_z, rows, width_y, group, block)

    def pair(length):
        return split_pair(jnp.asarray(sine(length), jnp.float32))

    x_high, x_low = pair(width_x)
    y_high, y_low = pair(width_y)
    x_twice = jnp.concatenate([x_high, x_high], axis=1)
    w = jnp.concatenate(
        [
            jnp.concatenate([y_high, y_low], axis=1),
            jnp.concatenate([y_high, jnp.zeros_like(y_low)], axis=1),
        ],
        axis=0,
    )
    sides = jnp.asarray(eigen(width_x)[:, None] + eigen(width_y)[None, :], jnp.float32)
    f32, b16 = jnp.float32, jnp.bfloat16
    flat = length_z * rows
    dma = pltpu.SemaphoreType.DMA
    vmem = pl.BlockSpec(memory_space=pltpu.VMEM)
    hbm = pl.BlockSpec(memory_space=pl.ANY)
    return pl.pallas_call(
        functools.partial(kernel, dims),
        out_shape=pltpu.VMEM((1, 5, depth, width_x, width_y), f32),
        in_specs=[pl.BlockSpec(memory_space=pltpu.SMEM)] + [hbm] * 7,
        out_specs=vmem,
        scratch_shapes=[
            pltpu.VMEM((depth, width_x, width_y), f32),
            pltpu.VMEM((depth, width_x, width_y), f32),
            pltpu.VMEM((5, depth, width_x, width_y), f32),
            pltpu.VMEM((width_x, 2 * width_x), b16),
            pltpu.VMEM((width_x, width_x), b16),
            pltpu.VMEM((2 * width_y, 2 * width_y), b16),
            pltpu.VMEM((width_x, width_y), f32),
            pltpu.VMEM((chunks, workers, 6, depth, rows, width_y), f32),
            pltpu.VMEM((chunks, spaces, 6, depth, rows, width_y), f32),
            pltpu.VMEM((chunks, flat, width_y), f32),
            pltpu.VMEM((chunks, flat, width_y), f32),
            pltpu.VMEM((chunks, flat, width_y), f32),
            pltpu.VMEM((8, width_y), f32),
            pltpu.VMEM((group, 8, width_y), f32),
            pltpu.VMEM((flat, width_y), f32),
            pltpu.VMEM((chunks, 4, flat, width_y), f32),
            pltpu.VMEM((chunks, 4, flat, width_y), f32),
            pltpu.VMEM((chunks, 4, flat, width_y), f32),
            pltpu.VMEM((chunks, group, 2, block, width_y), f32),
            pltpu.VMEM((chunks, group, 2, block, width_y), f32),
            pltpu.VMEM((chunks, group, block, width_y), f32),
            pltpu.VMEM((chunks, group, block, width_y), f32),
            pltpu.VMEM((chunks, group, 2, block, width_y), f32),
            pltpu.VMEM((chunks, group, 2, block, width_y), f32),
            pltpu.VMEM((chunks, 2, block, width_y), f32),
            pltpu.VMEM((chunks, 2, block, width_y), f32),
            pltpu.VMEM((chunks, spaces, 5, depth, rows, width_y), f32),
            pltpu.VMEM((chunks, workers, 5, depth, rows, width_y), f32),
            pltpu.VMEM((5, 2 * width_x, depth * width_y), b16),
            dma((7,)),
            dma((chunks, 2)),
            dma((chunks,)),
            dma((chunks, 2)),
            dma((chunks,)),
            dma((chunks,)),
            dma((chunks + 1,)),
            dma((14,)),
            pltpu.SemaphoreType.REGULAR((3,)),
        ],
        compiler_params=pltpu.CompilerParams(collective_id=0, has_side_effects=True),
    )(step_size, initial, start_guess, forcing, x_twice, x_low, w, sides)


def solution(mesh):
    in_specs = (
        P("space", None, None),
        P("tm", "space", None, None),
        P("tm", None, "space", None, None),
        P("tm"),
    )
    out_specs = P("tm", None, "space", None, None)
    return jax.shard_map(body, mesh=mesh, in_specs=in_specs, out_specs=out_specs, check_vma=False)
```

```python
import functools
import math

import jax
import jax.numpy as jnp
import numpy as np
from jax import lax
from jax.experimental import pallas as pl
from jax.experimental.pallas import tpu as pltpu
from jax.sharding import PartitionSpec as P

MESH = pl.DeviceIdType.MESH
CHUNKS = 4
GROUP = 8

def node_tables():
    radical = math.sqrt(3.0 / 7.0)
    node_times = [0.0, (1.0 - radical) / 2.0, 0.5, (1.0 + radical) / 2.0, 1.0]
    integrals = np.zeros((4, 5))
    for column in range(5):
        coeffs = [1.0]
        for other_index in range(5):
            if other_index == column:
                continue
            other_time = node_times[other_index]
            scaling = node_times[column] - other_time
            grown = [0.0] * (len(coeffs) + 1)
            for exponent in range(len(coeffs)):
                grown[exponent + 1] += coeffs[exponent] / scaling
                grown[exponent] -= coeffs[exponent] * other_time / scaling
            coeffs = grown
        for section in range(4):
            integrals[section, column] = sum(
                (
                    coeffs[exponent]
                    * (
                        node_times[section + 1] ** (exponent + 1)
                        - node_times[section] ** (exponent + 1)
                    )
                    / (exponent + 1)
                    for exponent in range(len(coeffs))
                )
            )
    coarse = [0.0, 0.5, 1.0]
    interp = np.zeros((5, 3))
    for column in range(3):
        for section in range(5):
            weight = 1.0
            for other_index in range(3):
                if other_index != column:
                    weight = (
                        weight
                        * (node_times[section] - coarse[other_index])
                        / (coarse[column] - coarse[other_index])
                    )
            interp[section, column] = weight
    return (np.array(node_times), integrals, interp)


def sine(length):
    k = np.arange(1, length + 1)
    phase = np.outer(k, k) % (2 * (length + 1))
    return math.sqrt(2.0 / (length + 1)) * np.sin(math.pi / (length + 1) * phase)


def eigen(length):
    return 2.0 - 2.0 * np.cos(math.pi / (length + 1) * np.arange(1, length + 1))


def split_pair(value):
    high = value.astype(jnp.bfloat16)
    return high, (value - high.astype(jnp.float32)).astype(jnp.bfloat16)


def dot(a, b):
    return jnp.dot(a, b, preferred_element_type=jnp.float32)


def along_y(field, w_ref):
    width = field.shape[1]
    both = dot(jnp.concatenate(split_pair(field), axis=1), w_ref[...])
    return both[:, :width] + both[:, width:]


def along_x(pair, high, x_ref, low_ref):
    return dot(x_ref[...], pair) + dot(low_ref[...], high)


def lateral(field, x_ref, low_ref, w_ref):
    depth, width_x, width_y = field.shape
    mixed = along_y(field.reshape(depth * width_x, width_y), w_ref)
    mixed = jnp.concatenate([mixed[z * width_x : (z + 1) * width_x] for z in range(depth)], axis=1)
    high, low = split_pair(mixed)
    out = along_x(jnp.concatenate([high, low], axis=0), high, x_ref, low_ref)
    return [out[:, z * width_y : (z + 1) * width_y] for z in range(depth)]


def z_sine(planes):
    count = len(planes)
    table = sine(count)
    half = (count + 1) // 2
    pairs = [
        (planes[z] + planes[count - 1 - z], planes[z] - planes[count - 1 - z])
        if z != count - 1 - z
        else (planes[z], None)
        for z in range(half)
    ]
    out = []
    for k in range(count):
        terms = [
            float(table[k, z]) * pairs[z][k % 2] for z in range(half) if pairs[z][k % 2] is not None
        ]
        total = terms[0]
        for term in terms[1:]:
            total = total + term
        out.append(total)
    return out


def weighted(weights, items):
    total = None
    for weight, item in zip(weights, items):
        weight = float(weight)
        if weight == 0.0 or item is None:
            continue
        term = item if weight == 1.0 else weight * item
        total = term if total is None else total + term
    return total


def sweep(rate, nodes, sources):
    times, integrals, _ = TABLES
    swept = [nodes[0]]
    for m in range(4):
        spacing = float(times[m + 1] - times[m])
        inner = weighted(integrals[m], nodes)
        if m > 0:
            inner = inner + spacing * (swept[m] - nodes[m])
        step = rate * inner
        if swept[m] is not None:
            step = step + swept[m]
        if sources is not None:
            step = step + sources[m]
        swept.append(step)
    first = list(integrals[0] + integrals[1])
    second = list(integrals[2] + integrals[3])
    first[0] -= 0.5
    second[2] -= 0.5
    left = rate * weighted(first, swept)
    right = rate * weighted(second, swept)
    if sources is not None:
        left = left + (sources[0] + sources[1])
        right = right + (sources[2] + sources[3])
    return swept, left, right


def corrected(swept, left, right, middle):
    interp = TABLES[2]
    ending = middle * left + right
    deltas = [None if swept[0] is None else -swept[0], left - swept[2], ending - swept[4]]
    return [
        None,
        swept[1] + weighted(interp[1], deltas),
        left,
        swept[3] + weighted(interp[3], deltas),
        ending,
    ]


def start_gains(middle):
    interp = TABLES[2]
    square = middle * middle
    return [
        None,
        float(interp[1, 0]) + float(interp[1, 1]) * middle + float(interp[1, 2]) * square,
        middle,
        float(interp[3, 0]) + float(interp[3, 1]) * middle + float(interp[3, 2]) * square,
        square,
    ]


def gains_of(rate):
    middle = 1.0 + 0.5 * rate
    gains = start_gains(middle)
    nodes = [jnp.ones_like(middle)] + gains[1:]
    swept, left, right = sweep(rate, nodes, None)
    return gains, corrected(swept, left, right, middle)


TABLES = node_tables()


def kernel(
    dims,
    step_ref, initial_hbm, guess_hbm, forcing_hbm, x_hbm, low_hbm, w_hbm, lateral_hbm,
    result_ref,
    initial, guess, forcing, x_ref, low_ref, w_ref, lateral_ref,
    in_send, in_recv, ghat, hhat, ell, own_step, steps,
    first_hat, gain_c, gain_d, part_b, z_send, z_recv, own_gain, own_cross, r_send, r_recv,
    s_send, s_recv, o_send, o_recv, mix,
    load_sem, in_rs, h_rs, z_rs, s_rs, r_rs, o_rs, sent, signals,
):
    spaces, workers, slices, chunks, depth, length_z, rows, width_y, group, block = dims
    me = lax.axis_index("space")
    place = lax.axis_index("tm")
    _, integrals, _ = TABLES
    width_x = workers * chunks * rows
    seat = me // 2
    sub = 16 if block % 16 == 0 else 8
    everyone = spaces - 2
    last_group = slices // group - 1
    family, mine = place // group, lax.rem(place, group)
    eldest = place - mine
    near_sem, next_sem, open_sem = (signals.at[i] for i in range(3))
    h_ss, step_ss, z_ss, s_ss, r_ss, o_ss, step_rs = (sent.at[i] for i in range(7))
    in_ss = [sent.at[7 + i] for i in range(4)]
    first_in_ss, first_in_rs, first_ss = (sent.at[11 + i] for i in range(3))
    helper = jnp.logical_and(family == 0, mine < chunks)

    barrier = pltpu.get_barrier_semaphore()
    odd = lax.rem(me, 2) == 1
    for i in range(1, spaces):
        peer = lax.rem(me + i, spaces)

        @pl.when(lax.rem(peer, 2) == 1)
        def _():
            pl.semaphore_signal(barrier, inc=1, device_id={"space": peer}, device_id_type=MESH)

    sources = (
        guess_hbm.at[0], w_hbm, x_hbm, low_hbm, forcing_hbm.at[0], initial_hbm, lateral_hbm
    )
    loads = [
        pltpu.make_async_copy(source, target, load_sem.at[i])
        for i, (source, target) in enumerate(
            zip(sources, (guess, w_ref, x_ref, low_ref, forcing, initial, lateral_ref))
        )
    ]
    for load in loads:
        load.start()
    load_guess, load_w, load_x, load_low, load_forcing, load_initial, load_lateral = loads

    step = step_ref[0]
    own_step[...] = jnp.full(own_step.shape, step, jnp.float32)
    steps[mine] = jnp.full(own_step.shape, step, jnp.float32)

    def bulk(ref, sem):
        pltpu.make_async_copy(ref, ref, sem).wait()

    def low_of(c, worker):
        return (c * workers + worker) * rows

    def put(field, slot):
        planes = lateral(field, x_ref, low_ref, w_ref)
        for target in range(workers):
            for c in range(chunks):
                low = low_of(c, target)
                for z in range(depth):
                    in_send[c, target, slot, z] = planes[z][low : low + rows]

    def keep(c, low, high):
        in_recv[c, me, low:high] = in_send[c, seat, low:high]

    def in_start(c, low, high, left, landed):
        for worker in range(workers):
            peer = 2 * worker + 1

            @pl.when(me != peer)
            def _():
                pltpu.make_async_remote_copy(
                    src_ref=in_send.at[c, worker, low:high],
                    dst_ref=in_recv.at[c, me, low:high],
                    send_sem=left,
                    recv_sem=landed,
                    device_id={"space": peer},
                    device_id_type=MESH,
                ).start()

    def by_role(action):
        pl.when(odd)(lambda: action(workers - 1))
        pl.when(jnp.logical_not(odd))(lambda: action(workers))

    def in_wait(c, low, high, landed):
        bulk(in_recv.at[c, 0 : spaces - 1, low:high], landed)

    load_guess.wait()
    load_w.wait()
    load_x.wait()
    load_low.wait()
    put(guess[...], 0)

    @pl.when(odd)
    def _():
        pl.semaphore_wait(barrier, spaces - 1)
        pl.semaphore_signal(near_sem, inc=1, device_id={"space": me - 1}, device_id_type=MESH)

    @pl.when(jnp.logical_not(odd))
    def _():
        pl.semaphore_wait(near_sem, 1)

    def guess_start(c):
        in_start(c, 0, 1, in_ss[0], in_rs.at[c, 0])

    for c in range(chunks // 2):
        guess_start(c)

    def greet(target):
        pl.semaphore_signal(barrier, inc=1, device_id={"tm": target}, device_id_type=MESH)

    @pl.when(me == 0)
    def _():
        pl.when(place > 0)(lambda: greet(place - 1))

        @pl.when(place == 0)
        def _():
            for other in range(1, min(chunks, group)):
                greet(other)

    def relatives(action):
        for i in range(1, group):
            action(lax.rem(mine + i, group))

    @pl.when(me == everyone)
    def _():
        relatives(lambda other: greet(eldest + other))
        pl.when(family > 0)(lambda: greet(place - group))

    def tell(sem):
        for worker in range(workers):
            pl.semaphore_signal(
                sem, inc=1, device_id={"space": 2 * worker + 1}, device_id_type=MESH
            )

    load_initial.wait()

    @pl.when(helper)
    def _():
        put(initial[...], 5)
        in_start(mine, 5, 6, first_in_ss, first_in_rs)
        pl.when(odd)(lambda: keep(mine, 5, 6))

    for c in range(chunks // 2, chunks):
        guess_start(c)
    load_forcing.wait()
    for m in range(4):
        put(step * weighted(integrals[m], [forcing[j] for j in range(5)]), m + 1)

    last_left = 3

    def forcing_start(c):
        in_start(c, 1, 5, in_ss[min(c + 1, last_left)], in_rs.at[c, 1])

    def forcing_left(c):
        by_role(lambda n: bulk(in_send.at[c, 0:n, 1:5], in_ss[c + 1]))

    forcing_start(0)

    def guess_left():
        by_role(lambda n: bulk(in_send.at[:, 0:n, 0:1], in_ss[0]))

    helping = jnp.logical_and(helper, place > 0)
    hands = jnp.logical_or(helping, place < slices - 1)

    @pl.when(jnp.logical_not(odd))
    def _():
        @pl.when(me == 0)
        def _():
            both = jnp.logical_and(helping, place < slices - 1)
            pl.when(both)(lambda: pl.semaphore_wait(barrier, 2))
            pl.when(jnp.logical_and(hands, jnp.logical_not(both)))(
                lambda: pl.semaphore_wait(barrier, 1)
            )
            pl.when(hands)(lambda: tell(next_sem))

        guess_left()
        for c in range(1, chunks):
            if 1 < c < last_left + 1:
                forcing_left(c - 2)
            forcing_start(c)

            if c == 2:
                @pl.when(me == everyone)
                def _():
                    pl.when(family < last_group)(lambda: pl.semaphore_wait(barrier, group))
                    pl.when(family == last_group)(lambda: pl.semaphore_wait(barrier, group - 1))
                    tell(open_sem)

    halves = ((0, 3), (3, 5))

    def o_groups(c):
        return halves if c == chunks - 1 else ((0, 5),)

    def o_start(c, number):
        low, high = o_groups(c)[number]
        for i in range(1, spaces):
            peer = lax.rem(me + i, spaces)
            pltpu.make_async_remote_copy(
                src_ref=o_send.at[c, peer, low:high],
                dst_ref=o_recv.at[c, seat, low:high],
                send_sem=o_ss,
                recv_sem=o_rs.at[c + number],
                device_id={"space": peer},
                device_id_type=MESH,
            ).start()

    def o_wait(c, number):
        low, high = o_groups(c)[number]
        by_role(lambda n: bulk(o_recv.at[c, 0:n, low:high], o_rs.at[c + number]))

    load_lateral.wait()

    @pl.when(odd)
    def _():
        for c in range(chunks):
            keep(c, 0, 5)

        z_eigen = eigen(length_z)
        for c in range(chunks):
            low = pl.multiple_of(low_of(c, seat), 8)
            base = lateral_ref[pl.ds(low, rows), :]
            for k in range(length_z):
                ell[c, k * rows : (k + 1) * rows] = -(base + float(z_eigen[k]))

        def table(i, carry):
            for c in range(chunks):
                at = pl.ds(pl.multiple_of(i * rows, 8), rows)
                gains, crossed = gains_of(step * ell[c, at])
                for m in range(1, 5):
                    gain_c[c, m - 1, at] = gains[m]
                    gain_d[c, m - 1, at] = crossed[m]
            return carry

        lax.fori_loop(0, length_z, table, 0)

        def planes_of(c, slot):
            return [in_recv[c, z // depth, slot, z % depth] for z in range(length_z)]

        guess_left()
        if chunks > 1:
            forcing_start(1)

        pl.when(hands)(lambda: pl.semaphore_wait(next_sem, 1))
        after = lax.rem(place + 1, slices)

        def hand(source, target, c, left):
            pltpu.make_async_remote_copy(
                src_ref=source,
                dst_ref=hhat.at[c],
                send_sem=left,
                recv_sem=h_rs.at[c],
                device_id={"tm": target},
                device_id_type=MESH,
            ).start()

        def hand_guess(c):
            in_wait(c, 0, 1, in_rs.at[c, 0])
            for k, plane in enumerate(z_sine(planes_of(c, 0))):
                ghat[c, k * rows : (k + 1) * rows] = plane
            pl.when(place < slices - 1)(lambda: hand(ghat.at[c], after, c, h_ss))

        for c in range(chunks // 2):
            hand_guess(c)

        @pl.when(helper)
        def _():
            in_wait(mine, 5, 6, first_in_rs)
            for k, plane in enumerate(z_sine(planes_of(mine, 5))):
                first_hat[k * rows : (k + 1) * rows] = plane

            @pl.when(place == 0)
            def _():
                hhat[0] = first_hat[...]

            pl.when(place > 0)(lambda: hand(first_hat, 0, mine, first_ss))

        def forcing_next(c):
            if c < chunks:
                if c < last_left + 1:
                    forcing_left(c - 2)
                forcing_start(c)

        forcing_next(2)
        for c in range(chunks // 2, chunks):
            hand_guess(c)
        for c in range(3, chunks):
            forcing_next(c)

        pl.semaphore_wait(open_sem, 1)
        relatives(
            lambda other: pltpu.make_async_remote_copy(
                src_ref=own_step,
                dst_ref=steps.at[mine],
                send_sem=step_ss,
                recv_sem=step_rs,
                device_id={"tm": eldest + other},
                device_id_type=MESH,
            ).start()
        )

        youngest = jnp.where(mine == group - 1, 1, 0)

        def z_start(c, other):
            pltpu.make_async_remote_copy(
                src_ref=z_send.at[c, other],
                dst_ref=z_recv.at[c, mine],
                send_sem=z_ss,
                recv_sem=z_rs.at[c, youngest],
                device_id={"tm": eldest + other},
                device_id_type=MESH,
            ).start()

        first = jnp.where(place == 0, 1.0, 0.0).astype(jnp.float32)

        def chunk(c):
            in_wait(c, 1, 5, in_rs.at[c, 1])
            if c == 0:
                pl.when(place > 0)(lambda: bulk(hhat.at[c], h_rs.at[c]))
            else:
                bulk(hhat.at[c], h_rs.at[c])
            fhat = [z_sine(planes_of(c, m + 1)) for m in range(4)]
            for m in range(4):
                for k in range(length_z):
                    part_b[c, m, k * rows : (k + 1) * rows] = fhat[m][k]

            def solve(i, carry):
                for part in range(block // sub):
                    at = pl.ds(pl.multiple_of(i * block + part * sub, 8), sub)
                    here = pl.ds(part * sub, sub)
                    rate = step * ell[c, at]
                    middle = 1.0 + 0.5 * rate
                    guess_hat, start = ghat[c, at], hhat[c, at]
                    sources = [part_b[c, m, at] for m in range(4)]
                    one = sweep(rate, [start] + [guess_hat] * 4, sources)
                    nodes = corrected(*one, middle)
                    rest = corrected(*sweep(rate, nodes, sources), middle)
                    for m in range(1, 5):
                        part_b[c, m - 1, at] = rest[m]
                    seen = first * start
                    gain, cross = gain_c[c, 3, at], gain_d[c, 3, at]
                    z_send[c, i, 0, here] = nodes[4] + gain * seen
                    z_send[c, i, 1, here] = rest[4] + (gain + cross) * seen
                return carry

            half = group // 2
            for i in [half] + [k for k in range(1, group) if k != half]:
                other = lax.rem(mine + i, group)
                solve(other, 0)
                pl.when(place < slices - 1)(lambda: z_start(c, other))
            solve(mine, 0)
            z_recv[c, mine] = z_send[c, mine]

        def own_tables(c):
            def one(p, carry):
                for part in range(block // sub):
                    at = pl.ds(pl.multiple_of(mine * block + part * sub, 8), sub)
                    here = pl.ds(part * sub, sub)
                    gains, crossed = gains_of(steps[p][0:1] * ell[c, at])
                    own_gain[c, p, here] = gains[4]
                    own_cross[c, p, here] = crossed[4]
                return carry

            lax.fori_loop(0, group, one, 0)

        def r_start(c, other):
            pltpu.make_async_remote_copy(
                src_ref=r_send.at[c, other],
                dst_ref=r_recv.at[c, mine],
                send_sem=r_ss,
                recv_sem=r_rs.at[c],
                device_id={"tm": eldest + other},
                device_id_type=MESH,
            ).start()

        def scan(c):
            if c == 0:
                bulk(steps.at[0 : group - 1], step_rs)
            own_tables(c)

            @pl.when(mine < group - 1)
            def _():
                if group > 2:
                    bulk(z_recv.at[c, 0 : group - 2], z_rs.at[c, 0])

            pl.when(mine == group - 1)(lambda: bulk(z_recv.at[c, 0 : group - 1], z_rs.at[c, 0]))
            pl.when(family > 0)(lambda: bulk(s_recv.at[c], s_rs.at[c]))

            def advance(p, lower, upper):
                gain = own_gain[c, p]
                return (
                    gain * lower + z_recv[c, p, 0],
                    gain * upper + own_cross[c, p] * lower + z_recv[c, p, 1],
                )

            lower, upper = (jnp.where(family > 0, s_recv[c, i], 0.0) for i in range(2))
            for p in range(group):
                r_send[c, p, 0] = lower
                r_send[c, p, 1] = upper
                if p < group - 1:
                    lower, upper = advance(p, lower, upper)

            @pl.when(family < last_group)
            def _():
                pl.when(mine < group - 1)(lambda: bulk(z_recv.at[c, 0], z_rs.at[c, 1]))
                final = advance(group - 1, r_send[c, group - 1, 0], r_send[c, group - 1, 1])
                s_send[c, 0], s_send[c, 1] = final
                pltpu.make_async_remote_copy(
                    src_ref=s_send.at[c],
                    dst_ref=s_recv.at[c],
                    send_sem=s_ss,
                    recv_sem=s_rs.at[c],
                    device_id={"tm": place + group},
                    device_id_type=MESH,
                ).start()

            relatives(lambda other: pl.when(eldest + other > 0)(lambda: r_start(c, other)))
            r_recv[c, mine] = r_send[c, mine]

        def give(c, lower, upper):
            for m in range(5):
                if m == 0:
                    value = upper
                else:
                    value = (
                        gain_c[c, m - 1] * upper + gain_d[c, m - 1] * lower + part_b[c, m - 1]
                    )
                planes = z_sine([value[k * rows : (k + 1) * rows] for k in range(length_z)])
                if c == chunks - 1:
                    tall = along_y(jnp.concatenate(planes, axis=0), w_ref)
                    planes = [tall[z * rows : (z + 1) * rows] for z in range(length_z)]
                for z in range(length_z):
                    o_send[c, z // depth, m, z % depth] = planes[z]
                for number, (_, high) in enumerate(o_groups(c)):
                    if high == m + 1:
                        o_start(c, number)
                o_recv[c, seat, m] = o_send[c, me, m]

        def give_first(c):
            own = hhat[c]
            give(c, own, own)

        def give_later(c):
            bulk(r_recv.at[c, 0 : group - 1], r_rs.at[c])
            give(c, *(r_recv[c, :, i].reshape(length_z * rows, width_y) for i in range(2)))

        early = max(0, chunks - 3)
        for c in range(chunks):
            chunk(c)
            if c == early:
                pl.when(place == group - 1)(lambda: scan(0))
            if c == max(0, chunks - 2):
                pl.when(place < group - 1)(lambda: scan(0))
        pl.when(family > 0)(lambda: scan(0))

        @pl.when(place == 0)
        def _():
            for c in range(1, chunks):
                scan(c)
                give_first(c - 1)
            give_first(chunks - 1)

        def later(lag):
            for c in range(1, chunks):
                scan(c)
                if c >= lag:
                    give_later(c - lag)
            for c in range(max(0, chunks - lag), chunks):
                give_later(c)

        soon = jnp.logical_and(family > 0, mine < group // 2)
        pl.when(soon)(lambda: later(1))
        pl.when(jnp.logical_and(place > 0, jnp.logical_not(soon)))(lambda: later(2))

    def unmix(c, low, high):
        stacked = jnp.concatenate(
            [
                o_recv[c, s, m, z]
                for m in range(low, high)
                for z in range(depth)
                for s in range(workers)
            ],
            axis=0,
        )
        tall = workers * rows
        mixed = stacked if c == chunks - 1 else along_y(stacked, w_ref)
        mixed_high, mixed_low = split_pair(mixed)
        for m in range(low, high):
            for z in range(depth):
                at = ((m - low) * depth + z) * tall
                lanes = slice(z * width_y, (z + 1) * width_y)
                mix[m, c * tall : (c + 1) * tall, lanes] = mixed_high[at : at + tall]
                mix[m, width_x + c * tall : width_x + (c + 1) * tall, lanes] = mixed_low[
                    at : at + tall
                ]

    for c in range(chunks - 1):
        o_wait(c, 0)
        unmix(c, 0, 5)
    for number, (low, high) in enumerate(halves):
        o_wait(chunks - 1, number)
        unmix(chunks - 1, low, high)
        for m in range(low, high):
            out = along_x(mix[m], mix[m, :width_x], x_ref, low_ref)
            for z in range(depth):
                result_ref[0, m, z] = out[:, z * width_y : (z + 1) * width_y]

    if chunks > 2:
        by_role(lambda n: bulk(in_send.at[2:chunks, 0:n, 1:5], in_ss[last_left]))
    pl.when(helper)(lambda: by_role(lambda n: bulk(in_send.at[0, 0:n, 5:6], first_in_ss)))

    @pl.when(odd)
    def _():
        pl.when(helping)(lambda: bulk(first_hat, first_ss))
        bulk(o_send.at[:, 0 : spaces - 1], o_ss)
        bulk(steps.at[0 : group - 1], step_ss)

        @pl.when(place < slices - 1)
        def _():
            bulk(ghat, h_ss)
            bulk(z_send.at[:, 0 : group - 1], z_ss)

        pl.when(family < last_group)(lambda: bulk(s_send, s_ss))
        fewer = jnp.logical_and(family == 0, place > 0)
        if group > 2:
            pl.when(fewer)(lambda: bulk(r_send.at[:, 0 : group - 2], r_ss))
        pl.when(jnp.logical_not(fewer))(lambda: bulk(r_send.at[:, 0 : group - 1], r_ss))


def body(initial, start_guess, forcing, step_size):
    depth, width_x, width_y = initial.shape
    spaces, slices = lax.axis_size("space"), lax.axis_size("tm")
    length_z = depth * spaces
    chunks = CHUNKS
    workers = spaces // 2
    rows = width_x // workers // chunks
    group = max(1, min(GROUP, slices // 2))
    block = length_z * rows // group
    dims = (spaces, workers, slices, chunks, depth, length_z, rows, width_y, group, block)

    def pair(length):
        return split_pair(jnp.asarray(sine(length), jnp.float32))

    x_high, x_low = pair(width_x)
    y_high, y_low = pair(width_y)
    x_twice = jnp.concatenate([x_high, x_high], axis=1)
    w = jnp.concatenate(
        [
            jnp.concatenate([y_high, y_low], axis=1),
            jnp.concatenate([y_high, jnp.zeros_like(y_low)], axis=1),
        ],
        axis=0,
    )
    sides = jnp.asarray(eigen(width_x)[:, None] + eigen(width_y)[None, :], jnp.float32)
    f32, b16 = jnp.float32, jnp.bfloat16
    flat = length_z * rows
    dma = pltpu.SemaphoreType.DMA
    vmem = pl.BlockSpec(memory_space=pltpu.VMEM)
    hbm = pl.BlockSpec(memory_space=pl.ANY)
    return pl.pallas_call(
        functools.partial(kernel, dims),
        out_shape=pltpu.VMEM((1, 5, depth, width_x, width_y), f32),
        in_specs=[pl.BlockSpec(memory_space=pltpu.SMEM)] + [hbm] * 7,
        out_specs=vmem,
        scratch_shapes=[
            pltpu.VMEM((depth, width_x, width_y), f32),
            pltpu.VMEM((depth, width_x, width_y), f32),
            pltpu.VMEM((5, depth, width_x, width_y), f32),
            pltpu.VMEM((width_x, 2 * width_x), b16),
            pltpu.VMEM((width_x, width_x), b16),
            pltpu.VMEM((2 * width_y, 2 * width_y), b16),
            pltpu.VMEM((width_x, width_y), f32),
            pltpu.VMEM((chunks, workers, 6, depth, rows, width_y), f32),
            pltpu.VMEM((chunks, spaces, 6, depth, rows, width_y), f32),
            pltpu.VMEM((chunks, flat, width_y), f32),
            pltpu.VMEM((chunks, flat, width_y), f32),
            pltpu.VMEM((chunks, flat, width_y), f32),
            pltpu.VMEM((8, width_y), f32),
            pltpu.VMEM((group, 8, width_y), f32),
            pltpu.VMEM((flat, width_y), f32),
            pltpu.VMEM((chunks, 4, flat, width_y), f32),
            pltpu.VMEM((chunks, 4, flat, width_y), f32),
            pltpu.VMEM((chunks, 4, flat, width_y), f32),
            pltpu.VMEM((chunks, group, 2, block, width_y), f32),
            pltpu.VMEM((chunks, group, 2, block, width_y), f32),
            pltpu.VMEM((chunks, group, block, width_y), f32),
            pltpu.VMEM((chunks, group, block, width_y), f32),
            pltpu.VMEM((chunks, group, 2, block, width_y), f32),
            pltpu.VMEM((chunks, group, 2, block, width_y), f32),
            pltpu.VMEM((chunks, 2, block, width_y), f32),
            pltpu.VMEM((chunks, 2, block, width_y), f32),
            pltpu.VMEM((chunks, spaces, 5, depth, rows, width_y), f32),
            pltpu.VMEM((chunks, workers, 5, depth, rows, width_y), f32),
            pltpu.VMEM((5, 2 * width_x, depth * width_y), b16),
            dma((7,)),
            dma((chunks, 2)),
            dma((chunks,)),
            dma((chunks, 2)),
            dma((chunks,)),
            dma((chunks,)),
            dma((chunks + 1,)),
            dma((14,)),
            pltpu.SemaphoreType.REGULAR((3,)),
        ],
        compiler_params=pltpu.CompilerParams(collective_id=0, has_side_effects=True),
    )(step_size, initial, start_guess, forcing, x_twice, x_low, w, sides)


def solution(mesh):
    in_specs = (
        P("space", None, None),
        P("tm", "space", None, None),
        P("tm", None, "space", None, None),
        P("tm"),
    )
    out_specs = P("tm", None, "space", None, None)
    return jax.shard_map(body, mesh=mesh, in_specs=in_specs, out_specs=out_specs, check_vma=False)
```

```python
import functools
import math

import jax
import jax.numpy as jnp
import numpy as np
from jax import lax
from jax.experimental import pallas as pl
from jax.experimental.pallas import tpu as pltpu
from jax.sharding import PartitionSpec as P

MESH = pl.DeviceIdType.MESH
CHUNKS = 4
GROUP = 8

def node_tables():
    radical = math.sqrt(3.0 / 7.0)
    node_times = [0.0, (1.0 - radical) / 2.0, 0.5, (1.0 + radical) / 2.0, 1.0]
    integrals = np.zeros((4, 5))
    for column in range(5):
        coeffs = [1.0]
        for other_index in range(5):
            if other_index == column:
                continue
            other_time = node_times[other_index]
            scaling = node_times[column] - other_time
            grown = [0.0] * (len(coeffs) + 1)
            for exponent in range(len(coeffs)):
                grown[exponent + 1] += coeffs[exponent] / scaling
                grown[exponent] -= coeffs[exponent] * other_time / scaling
            coeffs = grown
        for section in range(4):
            integrals[section, column] = sum(
                (
                    coeffs[exponent]
                    * (
                        node_times[section + 1] ** (exponent + 1)
                        - node_times[section] ** (exponent + 1)
                    )
                    / (exponent + 1)
                    for exponent in range(len(coeffs))
                )
            )
    coarse = [0.0, 0.5, 1.0]
    interp = np.zeros((5, 3))
    for column in range(3):
        for section in range(5):
            weight = 1.0
            for other_index in range(3):
                if other_index != column:
                    weight = (
                        weight
                        * (node_times[section] - coarse[other_index])
                        / (coarse[column] - coarse[other_index])
                    )
            interp[section, column] = weight
    return (np.array(node_times), integrals, interp)


def sine(length):
    k = np.arange(1, length + 1)
    phase = np.outer(k, k) % (2 * (length + 1))
    return math.sqrt(2.0 / (length + 1)) * np.sin(math.pi / (length + 1) * phase)


def eigen(length):
    return 2.0 - 2.0 * np.cos(math.pi / (length + 1) * np.arange(1, length + 1))


def split_pair(value):
    high = value.astype(jnp.bfloat16)
    return high, (value - high.astype(jnp.float32)).astype(jnp.bfloat16)


def dot(a, b):
    return jnp.dot(a, b, preferred_element_type=jnp.float32)


def along_y(field, w_ref):
    width = field.shape[1]
    both = dot(jnp.concatenate(split_pair(field), axis=1), w_ref[...])
    return both[:, :width] + both[:, width:]


def along_x(pair, high, x_ref, low_ref):
    return dot(x_ref[...], pair) + dot(low_ref[...], high)


def lateral(field, x_ref, low_ref, w_ref):
    depth, width_x, width_y = field.shape
    mixed = along_y(field.reshape(depth * width_x, width_y), w_ref)
    mixed = jnp.concatenate([mixed[z * width_x : (z + 1) * width_x] for z in range(depth)], axis=1)
    high, low = split_pair(mixed)
    out = along_x(jnp.concatenate([high, low], axis=0), high, x_ref, low_ref)
    return [out[:, z * width_y : (z + 1) * width_y] for z in range(depth)]


def z_sine(planes):
    count = len(planes)
    table = sine(count)
    half = (count + 1) // 2
    pairs = [
        (planes[z] + planes[count - 1 - z], planes[z] - planes[count - 1 - z])
        if z != count - 1 - z
        else (planes[z], None)
        for z in range(half)
    ]
    out = []
    for k in range(count):
        terms = [
            float(table[k, z]) * pairs[z][k % 2] for z in range(half) if pairs[z][k % 2] is not None
        ]
        total = terms[0]
        for term in terms[1:]:
            total = total + term
        out.append(total)
    return out


def weighted(weights, items):
    total = None
    for weight, item in zip(weights, items):
        weight = float(weight)
        if weight == 0.0 or item is None:
            continue
        term = item if weight == 1.0 else weight * item
        total = term if total is None else total + term
    return total


def sweep(rate, nodes, sources):
    times, integrals, _ = TABLES
    swept = [nodes[0]]
    for m in range(4):
        spacing = float(times[m + 1] - times[m])
        inner = weighted(integrals[m], nodes)
        if m > 0:
            inner = inner + spacing * (swept[m] - nodes[m])
        step = rate * inner
        if swept[m] is not None:
            step = step + swept[m]
        if sources is not None:
            step = step + sources[m]
        swept.append(step)
    first = list(integrals[0] + integrals[1])
    second = list(integrals[2] + integrals[3])
    first[0] -= 0.5
    second[2] -= 0.5
    left = rate * weighted(first, swept)
    right = rate * weighted(second, swept)
    if sources is not None:
        left = left + (sources[0] + sources[1])
        right = right + (sources[2] + sources[3])
    return swept, left, right


def corrected(swept, left, right, middle):
    interp = TABLES[2]
    ending = middle * left + right
    deltas = [None if swept[0] is None else -swept[0], left - swept[2], ending - swept[4]]
    return [
        None,
        swept[1] + weighted(interp[1], deltas),
        left,
        swept[3] + weighted(interp[3], deltas),
        ending,
    ]


def start_gains(middle):
    interp = TABLES[2]
    square = middle * middle
    return [
        None,
        float(interp[1, 0]) + float(interp[1, 1]) * middle + float(interp[1, 2]) * square,
        middle,
        float(interp[3, 0]) + float(interp[3, 1]) * middle + float(interp[3, 2]) * square,
        square,
    ]


def gains_of(rate):
    middle = 1.0 + 0.5 * rate
    gains = start_gains(middle)
    nodes = [jnp.ones_like(middle)] + gains[1:]
    swept, left, right = sweep(rate, nodes, None)
    return gains, corrected(swept, left, right, middle)


TABLES = node_tables()


def kernel(
    dims,
    step_ref, initial_hbm, guess_hbm, forcing_hbm, x_hbm, low_hbm, w_hbm, lateral_hbm,
    result_ref,
    initial, guess, forcing, x_ref, low_ref, w_ref, lateral_ref,
    in_send, in_recv, ghat, hhat, ell, own_step, steps,
    first_hat, gain_c, gain_d, part_b, z_send, z_recv, own_gain, own_cross, r_send, r_recv,
    s_send, s_recv, o_send, o_recv, mix,
    load_sem, in_rs, h_rs, z_rs, s_rs, r_rs, o_rs, sent, signals,
):
    spaces, workers, slices, chunks, depth, length_z, rows, width_y, group, block = dims
    me = lax.axis_index("space")
    place = lax.axis_index("tm")
    _, integrals, _ = TABLES
    width_x = workers * chunks * rows
    seat = me // 2
    sub = 16 if block % 16 == 0 else 8
    everyone = spaces - 2
    last_group = slices // group - 1
    family, mine = place // group, lax.rem(place, group)
    eldest = place - mine
    near_sem, next_sem, open_sem = (signals.at[i] for i in range(3))
    h_ss, step_ss, z_ss, s_ss, r_ss, o_ss, step_rs = (sent.at[i] for i in range(7))
    in_ss = [sent.at[7 + i] for i in range(4)]
    first_in_ss, first_in_rs, first_ss = (sent.at[11 + i] for i in range(3))
    helper = jnp.logical_and(family == 0, mine < chunks)

    barrier = pltpu.get_barrier_semaphore()
    odd = lax.rem(me, 2) == 1
    for i in range(1, spaces):
        peer = lax.rem(me + i, spaces)

        @pl.when(lax.rem(peer, 2) == 1)
        def _():
            pl.semaphore_signal(barrier, inc=1, device_id={"space": peer}, device_id_type=MESH)

    sources = (
        guess_hbm.at[0], w_hbm, x_hbm, low_hbm, forcing_hbm.at[0], initial_hbm, lateral_hbm
    )
    loads = [
        pltpu.make_async_copy(source, target, load_sem.at[i])
        for i, (source, target) in enumerate(
            zip(sources, (guess, w_ref, x_ref, low_ref, forcing, initial, lateral_ref))
        )
    ]
    for load in loads:
        load.start()
    load_guess, load_w, load_x, load_low, load_forcing, load_initial, load_lateral = loads

    step = step_ref[0]
    own_step[...] = jnp.full(own_step.shape, step, jnp.float32)
    steps[mine] = jnp.full(own_step.shape, step, jnp.float32)

    def bulk(ref, sem):
        pltpu.make_async_copy(ref, ref, sem).wait()

    def low_of(c, worker):
        return (c * workers + worker) * rows

    def put(field, slot):
        planes = lateral(field, x_ref, low_ref, w_ref)
        for target in range(workers):
            for c in range(chunks):
                low = low_of(c, target)
                for z in range(depth):
                    in_send[c, target, slot, z] = planes[z][low : low + rows]

    def keep(c, low, high):
        in_recv[c, me, low:high] = in_send[c, seat, low:high]

    def in_start(c, low, high, left, landed):
        for worker in range(workers):
            peer = 2 * worker + 1

            @pl.when(me != peer)
            def _():
                pltpu.make_async_remote_copy(
                    src_ref=in_send.at[c, worker, low:high],
                    dst_ref=in_recv.at[c, me, low:high],
                    send_sem=left,
                    recv_sem=landed,
                    device_id={"space": peer},
                    device_id_type=MESH,
                ).start()

    def by_role(action):
        pl.when(odd)(lambda: action(workers - 1))
        pl.when(jnp.logical_not(odd))(lambda: action(workers))

    def in_wait(c, low, high, landed):
        bulk(in_recv.at[c, 0 : spaces - 1, low:high], landed)

    load_guess.wait()
    load_w.wait()
    load_x.wait()
    load_low.wait()
    put(guess[...], 0)

    @pl.when(odd)
    def _():
        pl.semaphore_wait(barrier, spaces - 1)
        pl.semaphore_signal(near_sem, inc=1, device_id={"space": me - 1}, device_id_type=MESH)

    @pl.when(jnp.logical_not(odd))
    def _():
        pl.semaphore_wait(near_sem, 1)

    def guess_start(c):
        in_start(c, 0, 1, in_ss[0], in_rs.at[c, 0])

    for c in range(chunks // 2):
        guess_start(c)

    def greet(target):
        pl.semaphore_signal(barrier, inc=1, device_id={"tm": target}, device_id_type=MESH)

    @pl.when(me == 0)
    def _():
        pl.when(place > 0)(lambda: greet(place - 1))

        @pl.when(place == 0)
        def _():
            for other in range(1, min(chunks, group)):
                greet(other)

    def relatives(action):
        for i in range(1, group):
            action(lax.rem(mine + i, group))

    @pl.when(me == everyone)
    def _():
        relatives(lambda other: greet(eldest + other))
        pl.when(family > 0)(lambda: greet(place - group))

    def tell(sem):
        for worker in range(workers):
            pl.semaphore_signal(
                sem, inc=1, device_id={"space": 2 * worker + 1}, device_id_type=MESH
            )

    load_initial.wait()

    @pl.when(helper)
    def _():
        put(initial[...], 5)
        in_start(mine, 5, 6, first_in_ss, first_in_rs)
        pl.when(odd)(lambda: keep(mine, 5, 6))

    for c in range(chunks // 2, chunks):
        guess_start(c)
    load_forcing.wait()
    for m in range(4):
        put(step * weighted(integrals[m], [forcing[j] for j in range(5)]), m + 1)

    last_left = 3

    def forcing_start(c):
        in_start(c, 1, 5, in_ss[min(c + 1, last_left)], in_rs.at[c, 1])

    def forcing_left(c):
        by_role(lambda n: bulk(in_send.at[c, 0:n, 1:5], in_ss[c + 1]))

    forcing_start(0)

    def guess_left():
        by_role(lambda n: bulk(in_send.at[:, 0:n, 0:1], in_ss[0]))

    helping = jnp.logical_and(helper, place > 0)
    hands = jnp.logical_or(helping, place < slices - 1)

    @pl.when(jnp.logical_not(odd))
    def _():
        @pl.when(me == 0)
        def _():
            both = jnp.logical_and(helping, place < slices - 1)
            pl.when(both)(lambda: pl.semaphore_wait(barrier, 2))
            pl.when(jnp.logical_and(hands, jnp.logical_not(both)))(
                lambda: pl.semaphore_wait(barrier, 1)
            )
            pl.when(hands)(lambda: tell(next_sem))

        guess_left()
        for c in range(1, chunks):
            if 1 < c < last_left + 1:
                forcing_left(c - 2)
            forcing_start(c)

            if c == 2:
                @pl.when(me == everyone)
                def _():
                    pl.when(family < last_group)(lambda: pl.semaphore_wait(barrier, group))
                    pl.when(family == last_group)(lambda: pl.semaphore_wait(barrier, group - 1))
                    tell(open_sem)

    halves = ((0, 4), (4, 5))

    def o_groups(c):
        return halves if c == chunks - 1 else ((0, 5),)

    def o_start(c, number):
        low, high = o_groups(c)[number]
        for i in range(1, spaces):
            peer = lax.rem(me + i, spaces)
            pltpu.make_async_remote_copy(
                src_ref=o_send.at[c, peer, low:high],
                dst_ref=o_recv.at[c, seat, low:high],
                send_sem=o_ss,
                recv_sem=o_rs.at[c + number],
                device_id={"space": peer},
                device_id_type=MESH,
            ).start()

    def o_wait(c, number):
        low, high = o_groups(c)[number]
        by_role(lambda n: bulk(o_recv.at[c, 0:n, low:high], o_rs.at[c + number]))

    load_lateral.wait()

    @pl.when(odd)
    def _():
        for c in range(chunks):
            keep(c, 0, 5)

        z_eigen = eigen(length_z)
        for c in range(chunks):
            low = pl.multiple_of(low_of(c, seat), 8)
            base = lateral_ref[pl.ds(low, rows), :]
            for k in range(length_z):
                ell[c, k * rows : (k + 1) * rows] = -(base + float(z_eigen[k]))

        def table(i, carry):
            for c in range(chunks):
                at = pl.ds(pl.multiple_of(i * rows, 8), rows)
                gains, crossed = gains_of(step * ell[c, at])
                for m in range(1, 5):
                    gain_c[c, m - 1, at] = gains[m]
                    gain_d[c, m - 1, at] = crossed[m]
            return carry

        lax.fori_loop(0, length_z, table, 0)

        def planes_of(c, slot):
            return [in_recv[c, z // depth, slot, z % depth] for z in range(length_z)]

        guess_left()
        if chunks > 1:
            forcing_start(1)

        pl.when(hands)(lambda: pl.semaphore_wait(next_sem, 1))
        after = lax.rem(place + 1, slices)

        def hand(source, target, c, left):
            pltpu.make_async_remote_copy(
                src_ref=source,
                dst_ref=hhat.at[c],
                send_sem=left,
                recv_sem=h_rs.at[c],
                device_id={"tm": target},
                device_id_type=MESH,
            ).start()

        def hand_guess(c):
            in_wait(c, 0, 1, in_rs.at[c, 0])
            for k, plane in enumerate(z_sine(planes_of(c, 0))):
                ghat[c, k * rows : (k + 1) * rows] = plane
            pl.when(place < slices - 1)(lambda: hand(ghat.at[c], after, c, h_ss))

        for c in range(chunks // 2):
            hand_guess(c)

        @pl.when(helper)
        def _():
            in_wait(mine, 5, 6, first_in_rs)
            for k, plane in enumerate(z_sine(planes_of(mine, 5))):
                first_hat[k * rows : (k + 1) * rows] = plane

            @pl.when(place == 0)
            def _():
                hhat[0] = first_hat[...]

            pl.when(place > 0)(lambda: hand(first_hat, 0, mine, first_ss))

        def forcing_next(c):
            if c < chunks:
                if c < last_left + 1:
                    forcing_left(c - 2)
                forcing_start(c)

        forcing_next(2)
        for c in range(chunks // 2, chunks):
            hand_guess(c)
        for c in range(3, chunks):
            forcing_next(c)

        pl.semaphore_wait(open_sem, 1)
        relatives(
            lambda other: pltpu.make_async_remote_copy(
                src_ref=own_step,
                dst_ref=steps.at[mine],
                send_sem=step_ss,
                recv_sem=step_rs,
                device_id={"tm": eldest + other},
                device_id_type=MESH,
            ).start()
        )

        youngest = jnp.where(mine == group - 1, 1, 0)

        def z_start(c, other):
            pltpu.make_async_remote_copy(
                src_ref=z_send.at[c, other],
                dst_ref=z_recv.at[c, mine],
                send_sem=z_ss,
                recv_sem=z_rs.at[c, youngest],
                device_id={"tm": eldest + other},
                device_id_type=MESH,
            ).start()

        first = jnp.where(place == 0, 1.0, 0.0).astype(jnp.float32)

        def chunk(c):
            in_wait(c, 1, 5, in_rs.at[c, 1])
            if c == 0:
                pl.when(place > 0)(lambda: bulk(hhat.at[c], h_rs.at[c]))
            else:
                bulk(hhat.at[c], h_rs.at[c])
            fhat = [z_sine(planes_of(c, m + 1)) for m in range(4)]
            for m in range(4):
                for k in range(length_z):
                    part_b[c, m, k * rows : (k + 1) * rows] = fhat[m][k]

            def solve(i, carry):
                for part in range(block // sub):
                    at = pl.ds(pl.multiple_of(i * block + part * sub, 8), sub)
                    here = pl.ds(part * sub, sub)
                    rate = step * ell[c, at]
                    middle = 1.0 + 0.5 * rate
                    guess_hat, start = ghat[c, at], hhat[c, at]
                    sources = [part_b[c, m, at] for m in range(4)]
                    one = sweep(rate, [start] + [guess_hat] * 4, sources)
                    nodes = corrected(*one, middle)
                    rest = corrected(*sweep(rate, nodes, sources), middle)
                    for m in range(1, 5):
                        part_b[c, m - 1, at] = rest[m]
                    seen = first * start
                    gain, cross = gain_c[c, 3, at], gain_d[c, 3, at]
                    z_send[c, i, 0, here] = nodes[4] + gain * seen
                    z_send[c, i, 1, here] = rest[4] + (gain + cross) * seen
                return carry

            half = group // 2
            for i in [half] + [k for k in range(1, group) if k != half]:
                other = lax.rem(mine + i, group)
                solve(other, 0)
                pl.when(place < slices - 1)(lambda: z_start(c, other))
            solve(mine, 0)
            z_recv[c, mine] = z_send[c, mine]

        def own_tables(c):
            def one(p, carry):
                for part in range(block // sub):
                    at = pl.ds(pl.multiple_of(mine * block + part * sub, 8), sub)
                    here = pl.ds(part * sub, sub)
                    gains, crossed = gains_of(steps[p][0:1] * ell[c, at])
                    own_gain[c, p, here] = gains[4]
                    own_cross[c, p, here] = crossed[4]
                return carry

            lax.fori_loop(0, group, one, 0)

        def r_start(c, other):
            pltpu.make_async_remote_copy(
                src_ref=r_send.at[c, other],
                dst_ref=r_recv.at[c, mine],
                send_sem=r_ss,
                recv_sem=r_rs.at[c],
                device_id={"tm": eldest + other},
                device_id_type=MESH,
            ).start()

        def scan(c):
            if c == 0:
                bulk(steps.at[0 : group - 1], step_rs)
            own_tables(c)

            @pl.when(mine < group - 1)
            def _():
                if group > 2:
                    bulk(z_recv.at[c, 0 : group - 2], z_rs.at[c, 0])

            pl.when(mine == group - 1)(lambda: bulk(z_recv.at[c, 0 : group - 1], z_rs.at[c, 0]))
            pl.when(family > 0)(lambda: bulk(s_recv.at[c], s_rs.at[c]))

            def advance(p, lower, upper):
                gain = own_gain[c, p]
                return (
                    gain * lower + z_recv[c, p, 0],
                    gain * upper + own_cross[c, p] * lower + z_recv[c, p, 1],
                )

            lower, upper = (jnp.where(family > 0, s_recv[c, i], 0.0) for i in range(2))
            for p in range(group):
                r_send[c, p, 0] = lower
                r_send[c, p, 1] = upper
                if p < group - 1:
                    lower, upper = advance(p, lower, upper)

            @pl.when(family < last_group)
            def _():
                pl.when(mine < group - 1)(lambda: bulk(z_recv.at[c, 0], z_rs.at[c, 1]))
                final = advance(group - 1, r_send[c, group - 1, 0], r_send[c, group - 1, 1])
                s_send[c, 0], s_send[c, 1] = final
                pltpu.make_async_remote_copy(
                    src_ref=s_send.at[c],
                    dst_ref=s_recv.at[c],
                    send_sem=s_ss,
                    recv_sem=s_rs.at[c],
                    device_id={"tm": place + group},
                    device_id_type=MESH,
                ).start()

            relatives(lambda other: pl.when(eldest + other > 0)(lambda: r_start(c, other)))
            r_recv[c, mine] = r_send[c, mine]

        def give(c, lower, upper):
            for m in range(5):
                if m == 0:
                    value = upper
                else:
                    value = (
                        gain_c[c, m - 1] * upper + gain_d[c, m - 1] * lower + part_b[c, m - 1]
                    )
                planes = z_sine([value[k * rows : (k + 1) * rows] for k in range(length_z)])
                if c == chunks - 1:
                    tall = along_y(jnp.concatenate(planes, axis=0), w_ref)
                    planes = [tall[z * rows : (z + 1) * rows] for z in range(length_z)]
                for z in range(length_z):
                    o_send[c, z // depth, m, z % depth] = planes[z]
                for number, (_, high) in enumerate(o_groups(c)):
                    if high == m + 1:
                        o_start(c, number)
                o_recv[c, seat, m] = o_send[c, me, m]

        def give_first(c):
            own = hhat[c]
            give(c, own, own)

        def give_later(c):
            bulk(r_recv.at[c, 0 : group - 1], r_rs.at[c])
            give(c, *(r_recv[c, :, i].reshape(length_z * rows, width_y) for i in range(2)))

        early = max(0, chunks - 3)
        for c in range(chunks):
            chunk(c)
            if c == early:
                pl.when(place == group - 1)(lambda: scan(0))
            if c == max(0, chunks - 2):
                pl.when(place < group - 1)(lambda: scan(0))
        pl.when(family > 0)(lambda: scan(0))

        @pl.when(place == 0)
        def _():
            for c in range(1, chunks):
                scan(c)
                give_first(c - 1)
            give_first(chunks - 1)

        def later(lag):
            for c in range(1, chunks):
                scan(c)
                if c >= lag:
                    give_later(c - lag)
            for c in range(max(0, chunks - lag), chunks):
                give_later(c)

        soon = jnp.logical_and(family > 0, mine < group - 1)
        pl.when(soon)(lambda: later(1))
        pl.when(jnp.logical_and(place > 0, jnp.logical_not(soon)))(lambda: later(2))

    def unmix(c, low, high):
        stacked = jnp.concatenate(
            [
                o_recv[c, s, m, z]
                for m in range(low, high)
                for z in range(depth)
                for s in range(workers)
            ],
            axis=0,
        )
        tall = workers * rows
        mixed = stacked if c == chunks - 1 else along_y(stacked, w_ref)
        mixed_high, mixed_low = split_pair(mixed)
        for m in range(low, high):
            for z in range(depth):
                at = ((m - low) * depth + z) * tall
                lanes = slice(z * width_y, (z + 1) * width_y)
                mix[m, c * tall : (c + 1) * tall, lanes] = mixed_high[at : at + tall]
                mix[m, width_x + c * tall : width_x + (c + 1) * tall, lanes] = mixed_low[
                    at : at + tall
                ]

    for c in range(chunks - 1):
        o_wait(c, 0)
        unmix(c, 0, 5)
    for number, (low, high) in enumerate(halves):
        o_wait(chunks - 1, number)
        unmix(chunks - 1, low, high)
        for m in range(low, high):
            out = along_x(mix[m], mix[m, :width_x], x_ref, low_ref)
            for z in range(depth):
                result_ref[0, m, z] = out[:, z * width_y : (z + 1) * width_y]

    if chunks > 2:
        by_role(lambda n: bulk(in_send.at[2:chunks, 0:n, 1:5], in_ss[last_left]))
    pl.when(helper)(lambda: by_role(lambda n: bulk(in_send.at[0, 0:n, 5:6], first_in_ss)))

    @pl.when(odd)
    def _():
        pl.when(helping)(lambda: bulk(first_hat, first_ss))
        bulk(o_send.at[:, 0 : spaces - 1], o_ss)
        bulk(steps.at[0 : group - 1], step_ss)

        @pl.when(place < slices - 1)
        def _():
            bulk(ghat, h_ss)
            bulk(z_send.at[:, 0 : group - 1], z_ss)

        pl.when(family < last_group)(lambda: bulk(s_send, s_ss))
        fewer = jnp.logical_and(family == 0, place > 0)
        if group > 2:
            pl.when(fewer)(lambda: bulk(r_send.at[:, 0 : group - 2], r_ss))
        pl.when(jnp.logical_not(fewer))(lambda: bulk(r_send.at[:, 0 : group - 1], r_ss))


def body(initial, start_guess, forcing, step_size):
    depth, width_x, width_y = initial.shape
    spaces, slices = lax.axis_size("space"), lax.axis_size("tm")
    length_z = depth * spaces
    chunks = CHUNKS
    workers = spaces // 2
    rows = width_x // workers // chunks
    group = max(1, min(GROUP, slices // 2))
    block = length_z * rows // group
    dims = (spaces, workers, slices, chunks, depth, length_z, rows, width_y, group, block)

    def pair(length):
        return split_pair(jnp.asarray(sine(length), jnp.float32))

    x_high, x_low = pair(width_x)
    y_high, y_low = pair(width_y)
    x_twice = jnp.concatenate([x_high, x_high], axis=1)
    w = jnp.concatenate(
        [
            jnp.concatenate([y_high, y_low], axis=1),
            jnp.concatenate([y_high, jnp.zeros_like(y_low)], axis=1),
        ],
        axis=0,
    )
    sides = jnp.asarray(eigen(width_x)[:, None] + eigen(width_y)[None, :], jnp.float32)
    f32, b16 = jnp.float32, jnp.bfloat16
    flat = length_z * rows
    dma = pltpu.SemaphoreType.DMA
    vmem = pl.BlockSpec(memory_space=pltpu.VMEM)
    hbm = pl.BlockSpec(memory_space=pl.ANY)
    return pl.pallas_call(
        functools.partial(kernel, dims),
        out_shape=pltpu.VMEM((1, 5, depth, width_x, width_y), f32),
        in_specs=[pl.BlockSpec(memory_space=pltpu.SMEM)] + [hbm] * 7,
        out_specs=vmem,
        scratch_shapes=[
            pltpu.VMEM((depth, width_x, width_y), f32),
            pltpu.VMEM((depth, width_x, width_y), f32),
            pltpu.VMEM((5, depth, width_x, width_y), f32),
            pltpu.VMEM((width_x, 2 * width_x), b16),
            pltpu.VMEM((width_x, width_x), b16),
            pltpu.VMEM((2 * width_y, 2 * width_y), b16),
            pltpu.VMEM((width_x, width_y), f32),
            pltpu.VMEM((chunks, workers, 6, depth, rows, width_y), f32),
            pltpu.VMEM((chunks, spaces, 6, depth, rows, width_y), f32),
            pltpu.VMEM((chunks, flat, width_y), f32),
            pltpu.VMEM((chunks, flat, width_y), f32),
            pltpu.VMEM((chunks, flat, width_y), f32),
            pltpu.VMEM((8, width_y), f32),
            pltpu.VMEM((group, 8, width_y), f32),
            pltpu.VMEM((flat, width_y), f32),
            pltpu.VMEM((chunks, 4, flat, width_y), f32),
            pltpu.VMEM((chunks, 4, flat, width_y), f32),
            pltpu.VMEM((chunks, 4, flat, width_y), f32),
            pltpu.VMEM((chunks, group, 2, block, width_y), f32),
            pltpu.VMEM((chunks, group, 2, block, width_y), f32),
            pltpu.VMEM((chunks, group, block, width_y), f32),
            pltpu.VMEM((chunks, group, block, width_y), f32),
            pltpu.VMEM((chunks, group, 2, block, width_y), f32),
            pltpu.VMEM((chunks, group, 2, block, width_y), f32),
            pltpu.VMEM((chunks, 2, block, width_y), f32),
            pltpu.VMEM((chunks, 2, block, width_y), f32),
            pltpu.VMEM((chunks, spaces, 5, depth, rows, width_y), f32),
            pltpu.VMEM((chunks, workers, 5, depth, rows, width_y), f32),
            pltpu.VMEM((5, 2 * width_x, depth * width_y), b16),
            dma((7,)),
            dma((chunks, 2)),
            dma((chunks,)),
            dma((chunks, 2)),
            dma((chunks,)),
            dma((chunks,)),
            dma((chunks + 1,)),
            dma((14,)),
            pltpu.SemaphoreType.REGULAR((3,)),
        ],
        compiler_params=pltpu.CompilerParams(collective_id=0, has_side_effects=True),
    )(step_size, initial, start_guess, forcing, x_twice, x_low, w, sides)


def solution(mesh):
    in_specs = (
        P("space", None, None),
        P("tm", "space", None, None),
        P("tm", None, "space", None, None),
        P("tm"),
    )
    out_specs = P("tm", None, "space", None, None)
    return jax.shard_map(body, mesh=mesh, in_specs=in_specs, out_specs=out_specs, check_vma=False)
```
